32 devices in a mesh: batch: 2 (over x), dap: 16 (over z, y, core).
Axes of the slice: x: 2, y: 2, z: 4, core: 2. Of those that a mesh axis runs over, the one named last changes fastest.
Arguments:
- pair_act: bfloat16 [512, 256, 128], P(('batch', 'dap')), parts along dimension 0
- pair_mask: int32 [512, 256], P(('batch', 'dap')), parts along dimension 0
- msa_act: bfloat16 [64, 512, 256], P(None, ('batch', 'dap')), parts along dimension 1
- opm_norm: bfloat16 [2, 2, 256], replicated
- opm_w_in: bfloat16 [2, 256, 2, 32], replicated
- opm_b_in: bfloat16 [2, 2, 32], replicated
- opm_w_out: bfloat16 [2, 1024, 128], replicated
- opm_b_out: bfloat16 [2, 128], replicated
- tri_norm_in: bfloat16 [2, 2, 128], replicated
- tri_w_ab: bfloat16 [2, 128, 4, 128], replicated
- tri_b_ab: bfloat16 [2, 4, 128], replicated
- tri_w_gate: bfloat16 [2, 128, 128], replicated
- tri_b_gate: bfloat16 [2, 128], replicated
- tri_norm_out: bfloat16 [2, 2, 128], replicated
- tri_w_out: bfloat16 [2, 128, 128], replicated
- tri_b_out: bfloat16 [2, 128], replicated
Outputs:
- output: bfloat16 [512, 256, 128], P(('batch', 'dap')), parts along dimension 0
There are 2 independent parts. The reference program is written for one: setup_inputs(seed, part) draws one part's arguments, and reference() takes and returns one part's arrays. A program takes and returns all parts, laid end to end along the dimension named above; an argument that names none is the same for every part.
All inputs are finite; a program needn't handle non-finite values.
Results may differ from the reference program's by a relative error of at most 0.0106302.
Values are sent between devices in bfloat16 or wider.
A program may use at most 1 GiB of HBM per device.

```python
import jax
import jax.numpy as jnp
from jax import lax

RESIDUES = 256
MSA_ROWS = 64
PAIR_DIM = 128
TRI_DIM = 128
MSA_DIM = 256
OPM_DIM = 32
LAYERS = 2
ROW_BLOCK = 8

LN_EPS = 1e-5


def normal_draw(base_key, arr_shape, draw_scale):
    return (draw_scale * jax.random.normal(base_key, arr_shape, jnp.float32)).astype(jnp.bfloat16)


def norm_draw(base_key, arr_shape):
    noise_val = 0.3 * jax.random.normal(base_key, arr_shape, jnp.float32)
    return (noise_val + jnp.array([1.0, 0.0], jnp.float32)[None, :, None]).astype(jnp.bfloat16)


def setup_inputs(seed: int = 0, part: int = 0) -> dict:
    part_keys = jax.random.split(jax.random.fold_in(jax.random.key(seed), part), 6)
    weight_keys = jax.random.split(jax.random.key(seed + 1), 13)
    row_part = jax.random.normal(part_keys[0], (RESIDUES, 1, PAIR_DIM), jnp.float32)
    col_part = jax.random.normal(part_keys[1], (1, RESIDUES, PAIR_DIM), jnp.float32)
    pair_noise = jax.random.normal(part_keys[2], (RESIDUES, RESIDUES, PAIR_DIM), jnp.float32)
    pair_act = (0.6 * row_part + 0.6 * col_part + 0.5 * pair_noise).astype(jnp.bfloat16)
    profile = jax.random.normal(part_keys[3], (1, RESIDUES, MSA_DIM), jnp.float32)
    msa_noise = jax.random.normal(part_keys[4], (MSA_ROWS, RESIDUES, MSA_DIM), jnp.float32)
    msa_act = (0.8 * profile + 0.6 * msa_noise).astype(jnp.bfloat16)
    valid_len = RESIDUES // 2 + jax.random.randint(part_keys[5], (), 0, RESIDUES // 2 + 1)
    seq_valid = (jnp.arange(RESIDUES) < valid_len).astype(jnp.int32)
    pair_mask = seq_valid[:, None] * seq_valid[None, :]
    return {
        'pair_act': pair_act,
        'pair_mask': pair_mask,
        'msa_act': msa_act,
        'opm_norm': norm_draw(weight_keys[0], (LAYERS, 2, MSA_DIM)),
        'opm_w_in': normal_draw(weight_keys[1], (LAYERS, MSA_DIM, 2, OPM_DIM), MSA_DIM ** -0.5),
        'opm_b_in': normal_draw(weight_keys[2], (LAYERS, 2, OPM_DIM), 0.5),
        'opm_w_out': normal_draw(weight_keys[3], (LAYERS, OPM_DIM * OPM_DIM, PAIR_DIM), (OPM_DIM * OPM_DIM) ** -0.5),
        'opm_b_out': normal_draw(weight_keys[4], (LAYERS, PAIR_DIM), 0.5),
        'tri_norm_in': norm_draw(weight_keys[5], (LAYERS, 2, PAIR_DIM)),
        'tri_w_ab': normal_draw(weight_keys[6], (LAYERS, PAIR_DIM, 4, TRI_DIM), PAIR_DIM ** -0.5),
        'tri_b_ab': normal_draw(weight_keys[7], (LAYERS, 4, TRI_DIM), 0.3),
        'tri_w_gate': normal_draw(weight_keys[8], (LAYERS, PAIR_DIM, PAIR_DIM), PAIR_DIM ** -0.5),
        'tri_b_gate': normal_draw(weight_keys[9], (LAYERS, PAIR_DIM), 0.5),
        'tri_norm_out': norm_draw(weight_keys[10], (LAYERS, 2, TRI_DIM)),
        'tri_w_out': normal_draw(weight_keys[11], (LAYERS, TRI_DIM, PAIR_DIM), TRI_DIM ** -0.5),
        'tri_b_out': normal_draw(weight_keys[12], (LAYERS, PAIR_DIM), 0.5),
    }


def layer_norm(values, norm_gains):
    x_f32 = values.astype(jnp.float32)
    mean_val = jnp.mean(x_f32, axis=-1, keepdims=True)
    centered = x_f32 - mean_val
    var_val = jnp.mean(centered * centered, axis=-1, keepdims=True)
    scaled = centered * lax.rsqrt(var_val + LN_EPS)
    return (scaled * norm_gains[0].astype(jnp.float32) + norm_gains[1].astype(jnp.float32)).astype(jnp.bfloat16)


def outer_mean_update(pair_act, msa_act, norm_w, w_in, b_in, w_out, b_out):
    msa_norm = layer_norm(msa_act, norm_w).astype(jnp.float32)
    w_in_f = w_in.astype(jnp.float32)
    b_in_f = b_in.astype(jnp.float32)
    left_proj = (jnp.einsum('snm,mc->snc', msa_norm, w_in_f[:, 0, :]) + b_in_f[0]).astype(jnp.bfloat16).astype(jnp.float32)
    right_proj = (jnp.einsum('snm,mc->snc', msa_norm, w_in_f[:, 1, :]) + b_in_f[1]).astype(jnp.bfloat16).astype(jnp.float32)
    w_out_f = w_out.astype(jnp.float32).reshape(OPM_DIM, OPM_DIM, PAIR_DIM)
    b_out_f = b_out.astype(jnp.float32)
    num_blocks = RESIDUES // ROW_BLOCK
    left_blocks = jnp.moveaxis(left_proj.reshape(MSA_ROWS, num_blocks, ROW_BLOCK, OPM_DIM), 1, 0)
    pair_blocks = pair_act.reshape(num_blocks, ROW_BLOCK, RESIDUES, PAIR_DIM)

    def block_update(block_args):
        left_blk, pair_blk = block_args
        outer_prod = jnp.einsum('sic,sjd->ijcd', left_blk, right_proj) / MSA_ROWS
        outer_prod = outer_prod.astype(jnp.bfloat16).astype(jnp.float32)
        pair_upd = (jnp.einsum('ijcd,cdz->ijz', outer_prod, w_out_f) + b_out_f).astype(jnp.bfloat16)
        return (pair_blk.astype(jnp.float32) + pair_upd.astype(jnp.float32)).astype(jnp.bfloat16)

    return lax.map(block_update, (left_blocks, pair_blocks)).reshape(RESIDUES, RESIDUES, PAIR_DIM)


def triangle_update(pair_act, mask_f, norm_in, w_ab, b_ab, w_gate, b_gate, norm_out, w_out, b_out):
    num_blocks = RESIDUES // ROW_BLOCK
    pair_blocks = pair_act.reshape(num_blocks, ROW_BLOCK, RESIDUES, PAIR_DIM)
    mask_blocks = mask_f.reshape(num_blocks, ROW_BLOCK, RESIDUES)
    w_ab_f = w_ab.astype(jnp.float32)
    b_ab_f = b_ab.astype(jnp.float32)
    w_gate_f = w_gate.astype(jnp.float32)
    b_gate_f = b_gate.astype(jnp.float32)
    w_out_f = w_out.astype(jnp.float32)
    b_out_f = b_out.astype(jnp.float32)

    def project_block(block_args):
        pair_blk, mask_blk = block_args
        normed = layer_norm(pair_blk, norm_in).astype(jnp.float32)
        projected = jnp.einsum('ikz,zqc->qikc', normed, w_ab_f) + b_ab_f[:, None, None, :]
        mask_col = mask_blk[:, :, None]
        left_val = (mask_col * jax.nn.sigmoid(projected[1]) * projected[0]).astype(jnp.bfloat16)
        right_val = (mask_col * jax.nn.sigmoid(projected[3]) * projected[2]).astype(jnp.bfloat16)
        return left_val, right_val

    left_all, right_all = lax.map(project_block, (pair_blocks, mask_blocks))
    right_f = right_all.reshape(RESIDUES, RESIDUES, TRI_DIM).astype(jnp.float32)

    def update_block(block_args):
        pair_blk, left_blk = block_args
        normed = layer_norm(pair_blk, norm_in).astype(jnp.float32)
        gate_val = jax.nn.sigmoid(jnp.einsum('ikz,zy->iky', normed, w_gate_f) + b_gate_f)
        tri_prod = jnp.einsum('ikc,jkc->ijc', left_blk.astype(jnp.float32), right_f)
        prod_norm = layer_norm(tri_prod, norm_out).astype(jnp.float32)
        pair_upd = (jnp.einsum('ijc,cz->ijz', prod_norm, w_out_f) + b_out_f).astype(jnp.bfloat16)
        return (pair_blk.astype(jnp.float32) + gate_val * pair_upd.astype(jnp.float32)).astype(jnp.bfloat16)

    return lax.map(update_block, (pair_blocks, left_all)).reshape(RESIDUES, RESIDUES, PAIR_DIM)


def reference(pair_act, pair_mask, msa_act, opm_norm, opm_w_in, opm_b_in, opm_w_out, opm_b_out, tri_norm_in, tri_w_ab, tri_b_ab, tri_w_gate, tri_b_gate, tri_norm_out, tri_w_out, tri_b_out):
    mask_f = pair_mask.astype(jnp.float32)
    for layer_idx in range(LAYERS):
        pair_act = outer_mean_update(pair_act, msa_act, opm_norm[layer_idx], opm_w_in[layer_idx], opm_b_in[layer_idx], opm_w_out[layer_idx], opm_b_out[layer_idx])
        pair_act = triangle_update(pair_act, mask_f, tri_norm_in[layer_idx], tri_w_ab[layer_idx], tri_b_ab[layer_idx], tri_w_gate[layer_idx], tri_b_gate[layer_idx], tri_norm_out[layer_idx], tri_w_out[layer_idx], tri_b_out[layer_idx])
    return pair_act
```

```python
import functools
import jax
import jax.numpy as jnp
from jax import lax
from jax.sharding import PartitionSpec as P
from jax.experimental import pallas as pl
from jax.experimental.pallas import tpu as pltpu

EPS = 1e-5
MESH = pl.DeviceIdType.MESH
F32, BF16 = jnp.float32, jnp.bfloat16
NT = 8
CC = 16
NZ = 4

NTD = (((1,), (1,)), ((), ()))


def place():
    me = lax.axis_index('dap')
    return me // 4, (me // 2) % 2, me % 2


def dap_of(z, y, c):
    return (z * 2 + y) * 2 + c


def gather_kernel(b_ref, out_ref, send_i, recv_i, send_d, recv_d, own_sem):
    z, y, c = place()
    chip = z * 2 + y
    other = dap_of(z, y, 1 - c)

    def slot(ch, core):
        zz, yy = ch // 2, ch % 2
        return out_ref.at[:, :, pl.ds(pl.multiple_of(((yy * 4 + zz) * 2 + core) * 16, 16), 16), :]

    bar = pltpu.get_barrier_semaphore()
    for r in range(1, 8):
        pl.semaphore_signal(bar, inc=1, device_id={'dap': lax.rem(chip + r, 8) * 2 + c}, device_id_type=MESH)
    pl.semaphore_signal(bar, inc=1, device_id={'dap': other}, device_id_type=MESH)
    pl.semaphore_wait(bar, 8)

    def ici(r):
        return pltpu.make_async_remote_copy(
            b_ref, slot(chip, c), send_i.at[r], recv_i.at[r],
            device_id={'dap': lax.rem(chip + r, 8) * 2 + c}, device_id_type=MESH)

    def d2d(r):
        src = lax.rem(chip - r + 8, 8)
        return pltpu.make_async_remote_copy(
            b_ref if r == 0 else slot(src, c), slot(src, c), send_d.at[r], recv_d.at[r],
            device_id={'dap': other}, device_id_type=MESH)

    for r in range(1, 8):
        ici(r).start()
    d2d(0).start()
    mine = pltpu.make_async_copy(b_ref, slot(chip, c), own_sem)
    mine.start()
    for r in range(1, 8):
        ici(r).wait_recv()
        d2d(r).start()
    mine.wait()
    for r in range(1, 8):
        ici(r).wait_send()
    for r in range(8):
        d2d(r).wait()


def gather_b(b):
    return pl.pallas_call(
        gather_kernel,
        out_shape=jax.ShapeDtypeStruct((2, 16, 256, 128), BF16),
        in_specs=[pl.BlockSpec(memory_space=pltpu.VMEM)],
        out_specs=pl.BlockSpec(memory_space=pltpu.VMEM),
        scratch_shapes=[pltpu.SemaphoreType.DMA((8,))] * 4 + [pltpu.SemaphoreType.DMA],
        compiler_params=pltpu.CompilerParams(collective_id=0, has_side_effects=True),
        name='gather_b',
    )(b)


def layer_kernel(zt_ref, mask_ref, al_ref, bg_ref, wq_ref, wab_ref, bab_ref, wg_ref, wo_ref, cols_ref, no_ref,
                 out_ref,
                 q_ref, zn_ref, ast_ref, bst_ref, aown_ref, arecv_ref, b_ref, obuf_ref, osend_ref, ost_ref, on_ref,
                 sa, ra, sz, rz, sd, rd, so, ro):
    z, y, c = place()
    ypart = dap_of(z, 1 - y, c)
    cpart = dap_of(z, y, 1 - c)

    bar = pltpu.get_barrier_semaphore()
    pl.semaphore_signal(bar, inc=1, device_id={'dap': ypart}, device_id_type=MESH)
    pl.semaphore_signal(bar, inc=1, device_id={'dap': cpart}, device_id_type=MESH)

    @pl.when(z > 0)
    def _():
        pl.semaphore_signal(bar, inc=1, device_id={'dap': dap_of(z - 1, y, c)}, device_id_type=MESH)

    @pl.when(z < NZ - 1)
    def _():
        pl.semaphore_signal(bar, inc=1, device_id={'dap': dap_of(z + 1, y, c)}, device_id_type=MESH)

    @pl.loop(0, 16)
    def _(dp):
        bt = bg_ref[dp]
        for par in range(2):
            for h in range(2):
                rows = lax.dot_general(al_ref[pl.ds(par * 512 + h * 256, 256), :], bt, NTD, preferred_element_type=F32)
                rows = (rows * (1.0 / 64)).astype(BF16).reshape(8, 32, 256)
                q_ref[pl.ds(h * 8, 8), pl.ds(pl.multiple_of((dp * 2 + par) * 32, 32), 32), :] = rows

    wq = wq_ref

    def opm_row(i, _):
        upd = jnp.dot(wq[...], q_ref[i], preferred_element_type=F32) + cols_ref[:, 0:1]
        zi = (zt_ref[i].astype(F32) + upd.astype(BF16).astype(F32)).astype(BF16)
        out_ref[i] = zi
        x = zi.astype(F32)
        xc = x - jnp.mean(x, axis=0, keepdims=True)
        var = jnp.mean(xc * xc, axis=0, keepdims=True)
        zn_ref[i] = (xc * lax.rsqrt(var + EPS) * cols_ref[:, 1:2] + cols_ref[:, 2:3]).astype(BF16)
        return 0

    lax.fori_loop(0, 16, opm_row, 0)

    r_i = lax.broadcasted_iota(jnp.int32, (256, 256), 0)
    c_i = lax.broadcasted_iota(jnp.int32, (256, 256), 1)
    perm = ((r_i // 16 == c_i % 16) & (r_i % 16 == c_i // 16)).astype(F32).astype(BF16)

    def cp_a(t):
        return pltpu.make_async_remote_copy(aown_ref.at[t], arecv_ref.at[t], sa.at[t], ra.at[t],
                                            device_id={'dap': ypart}, device_id_type=MESH)

    def cp_o(t):
        return pltpu.make_async_remote_copy(osend_ref.at[t], obuf_ref.at[y, t], so.at[t], ro.at[t],
                                            device_id={'dap': ypart}, device_id_type=MESH)

    def cp_d(zs, t):
        return pltpu.make_async_remote_copy(b_ref.at[zs, c, t], b_ref.at[zs, c, t], sd.at[zs, t], rd.at[zs, t],
                                            device_id={'dap': cpart}, device_id_type=MESH)

    def cp_z(up, h, t):
        zs, zd = (z - h, z + 1) if up else (z + h, z - 1)
        return pltpu.make_async_remote_copy(b_ref.at[zs, c, t], b_ref.at[zs, c, t],
                                            sz.at[int(up), h, t], rz.at[int(up), h, t],
                                            device_id={'dap': dap_of(zd, y, c)}, device_id_type=MESH)

    def can_send(up, h):
        return (z - h >= 0) & (z + 1 < NZ) if up else (z + h < NZ) & (z - 1 >= 0)

    def can_recv(up, h):
        return z - h - 1 >= 0 if up else z + h + 1 < NZ

    def project(t, _):
        bias = jnp.broadcast_to(bab_ref[t], (64, 256))
        w = wab_ref[t]

        def row(i, _):
            p = jnp.dot(w, zn_ref[i], preferred_element_type=F32) + bias
            m = mask_ref[i]
            at = m * jax.nn.sigmoid(p[16:32]) * p[0:16]
            bt = m * jax.nn.sigmoid(p[48:64]) * p[32:48]
            ast_ref[pl.ds(pl.multiple_of(i * 16, 16), 16), :] = at.astype(BF16)
            bst_ref[pl.ds(pl.multiple_of(i * 16, 16), 16), :] = bt.astype(BF16)
            return 0

        lax.fori_loop(0, 16, row, 0, unroll=4)
        aown_ref[t] = jnp.dot(perm, ast_ref[...], preferred_element_type=F32).astype(BF16)
        b_ref[z, c, t] = jnp.dot(perm, bst_ref[...], preferred_element_type=F32).astype(BF16)

        @pl.when(t == 0)
        def _():
            n = 2 + (z > 0).astype(jnp.int32) + (z < NZ - 1).astype(jnp.int32)
            pl.semaphore_wait(bar, n)

        for up in (False, True):
            @pl.when(can_send(up, 0))
            def _():
                cp_z(up, 0, t).start()
        cp_a(t).start()
        cp_d(z, t).start()
        return 0

    lax.fori_loop(0, NT, project, 0)

    def arrive(h, t):
        for up in (False, True):
            @pl.when(can_recv(up, h))
            def _():
                zs = z - h - 1 if up else z + h + 1
                pltpu.make_async_remote_copy(b_ref.at[zs, c, t], b_ref.at[zs, c, t],
                                             sz.at[int(up), h, t], rz.at[int(up), h, t],
                                             device_id={'dap': cpart}, device_id_type=MESH).wait_recv()
                if h < NZ - 2:
                    @pl.when(can_send(up, h + 1))
                    def _():
                        cp_z(up, h + 1, t).start()
                cp_d(zs, t).start()

    for h in range(NZ - 2):
        @pl.loop(0, NT)
        def _(t):
            arrive(h, t)

    def multiply(t, _):
        arrive(NZ - 2, t)
        cp_a(t).wait_recv()
        for zs in range(NZ):
            pltpu.make_async_remote_copy(b_ref.at[zs, 1 - c, t], b_ref.at[zs, 1 - c, t], sd.at[zs, t], rd.at[zs, t],
                                         device_id={'dap': cpart}, device_id_type=MESH).wait_recv()
        for cc in range(CC):
            rs = pl.ds(cc * 16, 16)
            lhs = jnp.concatenate([aown_ref[t, rs, :], arecv_ref[t, rs, :]], axis=0)
            rhs = jnp.concatenate([b_ref[zs, k, t, rs, :] for zs in range(NZ) for k in range(2)], axis=0)
            o = lax.dot_general(lhs, rhs, NTD, preferred_element_type=F32)
            obuf_ref[y, t, rs, :] = o[0:16]
            osend_ref[t, rs, :] = o[16:32]
        cp_o(t).start()
        return 0

    lax.fori_loop(0, NT, multiply, 0)

    @pl.loop(0, NT)
    def _(t):
        cp_o(t).wait()
        cp_a(t).wait_send()
        for zs in range(NZ):
            cp_d(zs, t).wait_send()
        for up in (False, True):
            for h in range(NZ - 1):
                @pl.when(can_send(up, h))
                def _():
                    cp_z(up, h, t).wait_send()

    def load(t, cc, hh):
        return obuf_ref[hh, t, pl.ds(cc * 16, 16), :]

    zero = jnp.zeros((16, 128), F32)

    def add1(t, s):
        for cc in range(CC):
            s = tuple(s[hh] + load(t, cc, hh) for hh in range(2))
        return s

    tot = lax.fori_loop(0, NT, add1, (zero, zero))
    mean = tuple(s * (1.0 / 128) for s in tot)

    def add2(t, s):
        for cc in range(CC):
            d = tuple(load(t, cc, hh) - mean[hh] for hh in range(2))
            s = tuple(s[hh] + d[hh] * d[hh] for hh in range(2))
        return s

    sq = lax.fori_loop(0, NT, add2, (zero, zero))
    inv = tuple(lax.rsqrt(s * (1.0 / 128) + EPS) for s in sq)

    def norm(t, _):
        for cc in range(CC):
            for hh in range(2):
                v = (load(t, cc, hh) - mean[hh]) * inv[hh] * no_ref[0, t * CC + cc] + no_ref[1, t * CC + cc]
                ost_ref[pl.ds(cc * 16, 16), pl.ds(hh * 128, 128)] = v.astype(BF16)
        on = jnp.dot(perm, ost_ref[...], preferred_element_type=F32).astype(BF16)
        on_ref[:, pl.ds(pl.multiple_of(t * CC, 16), CC), :] = on.reshape(16, CC, 256)
        return 0

    lax.fori_loop(0, NT, norm, 0)

    def finish(i, _):
        u = (jnp.dot(wo_ref[...], on_ref[i], preferred_element_type=F32) + cols_ref[:, 3:4]).astype(BF16)
        g = jax.nn.sigmoid(jnp.dot(wg_ref[...], zn_ref[i], preferred_element_type=F32) + cols_ref[:, 4:5])
        out_ref[i] = (out_ref[i].astype(F32) + g * u.astype(F32)).astype(BF16)
        return 0

    lax.fori_loop(0, 16, finish, 0)


def layer(l, zt, mask, al, bg, wq, wab, bab, wg, wo, cols, no):
    vm = pl.BlockSpec(memory_space=pltpu.VMEM)
    dma = pltpu.SemaphoreType.DMA
    return pl.pallas_call(
        layer_kernel,
        out_shape=jax.ShapeDtypeStruct((16, 128, 256), BF16),
        in_specs=[vm] * 10 + [pl.BlockSpec(memory_space=pltpu.SMEM)],
        out_specs=vm,
        scratch_shapes=[
            pltpu.VMEM((16, 1024, 256), BF16),
            pltpu.VMEM((16, 128, 256), BF16),
            pltpu.VMEM((256, 256), BF16),
            pltpu.VMEM((256, 256), BF16),
            pltpu.VMEM((NT, 256, 256), BF16),
            pltpu.VMEM((NT, 256, 256), BF16),
            pltpu.VMEM((NZ, 2, NT, 256, 256), BF16),
            pltpu.VMEM((2, NT, 256, 128), F32),
            pltpu.VMEM((NT, 256, 128), F32),
            pltpu.VMEM((256, 256), BF16),
            pltpu.VMEM((16, 128, 256), BF16),
            dma((NT,)), dma((NT,)),
            dma((2, NZ - 1, NT)), dma((2, NZ - 1, NT)),
            dma((NZ, NT)), dma((NZ, NT)),
            dma((NT,)), dma((NT,)),
        ],
        compiler_params=pltpu.CompilerParams(collective_id=1 + l, has_side_effects=True),
        name=f'layer_{l}',
    )(zt, mask, al, bg, wq, wab, bab, wg, wo, cols, no)


def solution(mesh):
    pair_spec = P(('batch', 'dap'), None, None)
    mask_spec = P(('batch', 'dap'), None)
    msa_spec = P(None, ('batch', 'dap'), None)

    def device_fn(pair, mask, msa, opm_norm, opm_w_in, opm_b_in, opm_w_out, opm_b_out, tri_norm_in, tri_w_ab, tri_b_ab,
                  tri_w_gate, tri_b_gate, tri_norm_out, tri_w_out, tri_b_out):
        x = msa.astype(F32)
        xc = x - jnp.mean(x, axis=-1, keepdims=True)
        var = jnp.mean(xc * xc, axis=-1, keepdims=True)
        xh = xc * lax.rsqrt(var + EPS)
        nw = opm_norm.astype(F32)
        mn = (xh[None] * nw[:, 0][:, None, None] + nw[:, 1][:, None, None]).astype(BF16)
        bias = opm_b_in.astype(F32)
        b = (jnp.einsum('lmd,lsjm->ldjs', opm_w_in[:, :, 1], mn, preferred_element_type=F32)
             + bias[:, 1][:, :, None, None]).astype(BF16)
        b = b.reshape(2, 16, 2, 16, 64).transpose(0, 1, 3, 2, 4).reshape(2, 16, 16, 128)
        bg = gather_b(b)
        a = (jnp.einsum('lmc,lsim->lics', opm_w_in[:, :, 0], mn, preferred_element_type=F32)
             + bias[:, 0][:, None, :, None]).astype(BF16).reshape(2, 512, 64)
        al = jnp.concatenate([jnp.pad(a, ((0, 0), (0, 0), (0, 64))), jnp.pad(a, ((0, 0), (0, 0), (64, 0)))], axis=1)

        wq = opm_w_out.reshape(2, 32, 32, 128).transpose(0, 3, 2, 1).reshape(2, 128, 1024)
        wab = tri_w_ab.reshape(2, 128, 4, NT, CC).transpose(0, 3, 2, 4, 1).reshape(2, NT, 4 * CC, 128)
        bab = tri_b_ab.reshape(2, 4, NT, CC).transpose(0, 2, 1, 3).reshape(2, NT, 4 * CC, 1).astype(F32)
        wg = tri_w_gate.transpose(0, 2, 1)
        wo = tri_w_out.transpose(0, 2, 1)
        cols = jnp.stack([opm_b_out, tri_norm_in[:, 0], tri_norm_in[:, 1], tri_b_out, tri_b_gate], axis=-1).astype(F32)
        no = tri_norm_out.astype(F32)
        zt = pair.reshape(16, 4, 2, 32, 128).transpose(0, 4, 2, 1, 3).reshape(16, 128, 256)
        mf = mask.reshape(16, 4, 2, 32).transpose(0, 2, 1, 3).reshape(16, 1, 256).astype(F32)
        for l in range(2):
            zt = layer(l, zt, mf, al[l], bg[l], wq[l], wab[l], bab[l], wg[l], wo[l], cols[l], no[l])
        return zt.reshape(16, 128, 2, 4, 32).transpose(0, 3, 2, 4, 1).reshape(16, 256, 128)

    return jax.shard_map(device_fn, mesh=mesh, in_specs=(pair_spec, mask_spec, msa_spec) + (P(),) * 13,
                         out_specs=pair_spec, check_vma=False)
```

```python
import jax
import jax.numpy as jnp
from jax import lax
from jax.sharding import PartitionSpec as P
from jax.experimental import pallas as pl
from jax.experimental.pallas import tpu as pltpu

EPS = 1e-5
MESH = pl.DeviceIdType.MESH
F32, BF16 = jnp.float32, jnp.bfloat16
NL = 2
NT = 8
CC = 16
NZ = 4

NTD = (((1,), (1,)), ((), ()))


def place():
    me = lax.axis_index('dap')
    return me // 4, (me // 2) % 2, me % 2


def dap_of(z, y, c):
    return (z * 2 + y) * 2 + c


def sixteen(i):
    return pl.ds(pl.multiple_of(i * 16, 16), 16)


def kernel(zt_ref, mask_ref, al_ref, bown_ref, wq_ref, wab_ref, wg_ref, wo_ref, cols_ref, no_ref,
           out_ref,
           bg_ref, q_ref, wqt_ref, wabt_ref, wgt_ref, wot_ref, zn_ref, st_ref, aown_ref, arecv_ref, b_ref,
           obuf_ref, osend_ref, ost_ref, on_ref,
           sgi, rgi, sgd, rgd, sown, sa, ra, sz, rz, sd, rd, so, ro):
    z, y, c = place()
    chip = z * 2 + y
    ypart = dap_of(z, 1 - y, c)
    cpart = dap_of(z, y, 1 - c)

    bar = pltpu.get_barrier_semaphore()
    for r in range(1, 8):
        pl.semaphore_signal(bar, inc=1, device_id={'dap': lax.rem(chip + r, 8) * 2 + c}, device_id_type=MESH)
    pl.semaphore_signal(bar, inc=1, device_id={'dap': cpart}, device_id_type=MESH)
    pl.semaphore_wait(bar, 8)

    def bslot(l, ch, core):
        return bg_ref.at[l, :, sixteen((ch % 2 * 4 + ch // 2) * 2 + core), :]

    def g_ici(l, r):
        return pltpu.make_async_remote_copy(
            bown_ref.at[l], bslot(l, chip, c), sgi.at[l, r], rgi.at[l, r],
            device_id={'dap': lax.rem(chip + r, 8) * 2 + c}, device_id_type=MESH)

    def g_d2d(l, r):
        src = lax.rem(chip - r + 8, 8)
        return pltpu.make_async_remote_copy(
            bown_ref.at[l] if r == 0 else bslot(l, src, c), bslot(l, src, c), sgd.at[l, r], rgd.at[l, r],
            device_id={'dap': cpart}, device_id_type=MESH)

    def g_own(l):
        return pltpu.make_async_copy(bown_ref.at[l], bslot(l, chip, c), sown.at[l])

    def g_pass(l):
        for r in range(1, 8):
            g_ici(l, r).wait_recv()
            g_d2d(l, r).start()

    def g_finish(l):
        g_own(l).wait()
        for r in range(8):
            g_d2d(l, r).wait()
        for r in range(1, 8):
            g_ici(l, r).wait_send()

    def cp_a(l, t, kh):
        return pltpu.make_async_remote_copy(aown_ref.at[l, t, kh], arecv_ref.at[l, t, kh], sa.at[l, t, kh],
                                            ra.at[l, t, kh], device_id={'dap': ypart}, device_id_type=MESH)

    def cp_o(l, t):
        return pltpu.make_async_remote_copy(osend_ref.at[l, t], obuf_ref.at[l, y, t], so.at[l, t], ro.at[l, t],
                                            device_id={'dap': ypart}, device_id_type=MESH)

    def cp_d(l, zs, t, kh, core):
        blk = b_ref.at[l, zs, core, t, kh]
        return pltpu.make_async_remote_copy(blk, blk, sd.at[l, zs, t, kh], rd.at[l, zs, t, kh],
                                            device_id={'dap': cpart}, device_id_type=MESH)

    def cp_z(l, up, h, t, kh, zs, dev):
        blk = b_ref.at[l, zs, c, t, kh]
        return pltpu.make_async_remote_copy(blk, blk, sz.at[l, int(up), h, t, kh], rz.at[l, int(up), h, t, kh],
                                            device_id={'dap': dev}, device_id_type=MESH)

    def send_z(l, up, h, t, kh):
        zs, zd = (z - h, z + 1) if up else (z + h, z - 1)
        return cp_z(l, up, h, t, kh, zs, dap_of(zd, y, c))

    def can_send(up, h):
        return (z - h >= 0) & (z + 1 < NZ) if up else (z + h < NZ) & (z - 1 >= 0)

    def can_recv(up, h):
        return z - h - 1 >= 0 if up else z + h + 1 < NZ

    def arrive(l, h, t, kh):
        for up in (False, True):
            @pl.when(can_recv(up, h))
            def _():
                zs = z - h - 1 if up else z + h + 1
                cp_z(l, up, h, t, kh, zs, cpart).wait_recv()
                if h < NZ - 2:
                    @pl.when(can_send(up, h + 1))
                    def _():
                        send_z(l, up, h + 1, t, kh).start()
                cp_d(l, zs, t, kh, c).start()

    for l in range(NL):
        for r in range(1, 8):
            g_ici(l, r).start()
        g_d2d(l, 0).start()
        g_own(l).start()

    r_i = lax.broadcasted_iota(jnp.int32, (256, 256), 0)
    c_i = lax.broadcasted_iota(jnp.int32, (256, 256), 1)
    perm = ((r_i // 16 == c_i % 16) & (r_i % 16 == c_i // 16)).astype(F32).astype(BF16)

    def turn(w):
        return w.astype(F32).T.astype(BF16)

    def prepare(l):
        @pl.loop(0, 4)
        def _(blk):
            r2 = lax.broadcasted_iota(jnp.int32, (256, 1024), 0)
            k2 = lax.broadcasted_iota(jnp.int32, (256, 1024), 1)
            sel = ((k2 // 32 == r2 % 32) & (k2 % 32 == r2 // 32 + blk * 8)).astype(F32).astype(BF16)
            w = jnp.dot(sel, wq_ref[l], preferred_element_type=F32)
            wqt_ref[l, :, pl.ds(pl.multiple_of(blk * 256, 256), 256)] = w.T.astype(BF16)
        for qq in range(4):
            w = turn(wab_ref[l, :, qq * 128:(qq + 1) * 128])
            wabt_ref[l, :, qq * CC:(qq + 1) * CC, :] = w.reshape(NT, CC, 128)
        wgt_ref[l] = turn(wg_ref[l])
        wot_ref[l] = turn(wo_ref[l])

    def outer(l, kh):
        @pl.loop(0, 8)
        def _(dpp):
            half = pl.ds(kh * 128, 128)
            bt = jnp.concatenate([bg_ref[l, dpp * 2, half, :], bg_ref[l, dpp * 2 + 1, half, :]], axis=0)
            for par in range(2):
                for h in range(2):
                    rows = lax.dot_general(al_ref[l, pl.ds(par * 512 + h * 256, 256), :], bt, NTD,
                                           preferred_element_type=F32)
                    rows = (rows * (1.0 / 64)).astype(BF16).reshape(4, 2, 32, 256)
                    for e in range(2):
                        at = pl.ds(pl.multiple_of((dpp * 4 + e * 2 + par) * 32, 32), 32)
                        for i2 in range(2):
                            q_ref[pl.ds(h * 4, 4), at, i2 * 128:(i2 + 1) * 128] = rows[:, i2, :, e * 128:(e + 1) * 128]

        src = zt_ref if l == 0 else out_ref

        def rows(ip, _):
            upd = jnp.dot(wqt_ref[l], q_ref[ip], preferred_element_type=F32) + cols_ref[l, :, 0:1]
            zi = (src[kh, ip].astype(F32) + upd.astype(BF16).astype(F32)).astype(BF16)
            out_ref[kh, ip] = zi
            x = zi.astype(F32)
            xc = x - jnp.mean(x, axis=0, keepdims=True)
            var = jnp.mean(xc * xc, axis=0, keepdims=True)
            zn_ref[kh, ip] = (xc * lax.rsqrt(var + EPS) * cols_ref[l, :, 1:2] + cols_ref[l, :, 2:3]).astype(BF16)
            return 0

        lax.fori_loop(0, 8, rows, 0)

    def project(l, kh):
        def chunk(t, _):
            bias = jnp.concatenate([jnp.broadcast_to(cols_ref[l, sixteen(t), 5 + qq:6 + qq], (CC, 256))
                                    for qq in range(4)], axis=0)
            w = wabt_ref[l, t]

            def rows(ip, _):
                p = jnp.dot(w, zn_ref[kh, ip], preferred_element_type=F32) + bias
                m = mask_ref[kh, ip]
                at = (m * jax.nn.sigmoid(p[16:32]) * p[0:16]).astype(BF16)
                bt = (m * jax.nn.sigmoid(p[48:64]) * p[32:48]).astype(BF16)
                for i2 in range(2):
                    ln = slice(i2 * 128, (i2 + 1) * 128)
                    st_ref[sixteen(ip * 2 + i2), 0:128] = at[:, ln]
                    st_ref[sixteen(ip * 2 + i2), 128:256] = bt[:, ln]
                return 0

            lax.fori_loop(0, 8, rows, 0, unroll=4)
            ab = jnp.dot(perm, st_ref[...], preferred_element_type=F32).astype(BF16)
            aown_ref[l, t, kh] = ab[:, 0:128]
            b_ref[l, z, c, t, kh] = ab[:, 128:256]
            for up in (False, True):
                @pl.when(can_send(up, 0))
                def _():
                    send_z(l, up, 0, t, kh).start()
            cp_a(l, t, kh).start()
            cp_d(l, z, t, kh, c).start()
            return 0

        lax.fori_loop(0, NT, chunk, 0)

    def multiply(l, t):
        for kh in range(2):
            cp_a(l, t, kh).wait_recv()
            for zs in range(NZ):
                cp_d(l, zs, t, kh, 1 - c).wait_recv()
        for cc in range(CC):
            rs = pl.ds(cc * 16, 16)
            o = None
            lhs = jnp.concatenate([jnp.concatenate([r[l, t, kh, rs, :] for kh in range(2)], axis=1)
                                   for r in (aown_ref, arecv_ref)], axis=0)
            rhs = jnp.concatenate([jnp.concatenate([b_ref[l, zs, k, t, kh, rs, :] for kh in range(2)], axis=1)
                                   for zs in range(NZ) for k in range(2)], axis=0)
            o = lax.dot_general(lhs, rhs, NTD, preferred_element_type=F32)
            obuf_ref[l, y, t, rs, :] = o[0:16]
            osend_ref[l, t, rs, :] = o[16:32]
        cp_o(l, t).start()

    def drain(l):
        @pl.loop(0, NT)
        def _(t):
            cp_o(l, t).wait()
            for kh in range(2):
                cp_a(l, t, kh).wait_send()
                for zs in range(NZ):
                    cp_d(l, zs, t, kh, c).wait_send()
                for up in (False, True):
                    for h in range(NZ - 1):
                        @pl.when(can_send(up, h))
                        def _():
                            send_z(l, up, h, t, kh).wait_send()

    def finish(l):
        def load(t, cc, hh):
            return obuf_ref[l, hh, t, pl.ds(cc * 16, 16), :]

        zero = jnp.zeros((16, 128), F32)

        def add1(t, s):
            for cc in range(CC):
                s = tuple(s[hh] + load(t, cc, hh) for hh in range(2))
            return s

        tot = lax.fori_loop(0, NT, add1, (zero, zero))
        mean = tuple(s * (1.0 / 128) for s in tot)

        def add2(t, s):
            for cc in range(CC):
                d = tuple(load(t, cc, hh) - mean[hh] for hh in range(2))
                s = tuple(s[hh] + d[hh] * d[hh] for hh in range(2))
            return s

        sq = lax.fori_loop(0, NT, add2, (zero, zero))
        inv = tuple(lax.rsqrt(s * (1.0 / 128) + EPS) for s in sq)

        def norm(t, _):
            for cc in range(CC):
                for hh in range(2):
                    v = (load(t, cc, hh) - mean[hh]) * inv[hh] * no_ref[l, 0, t * CC + cc] + no_ref[l, 1, t * CC + cc]
                    ost_ref[pl.ds(cc * 16, 16), pl.ds(hh * 128, 128)] = v.astype(BF16)
            on = jnp.dot(perm, ost_ref[...], preferred_element_type=F32).astype(BF16).reshape(8, 2, CC, 256)
            for hh in range(2):
                for i2 in range(2):
                    on_ref[hh, :, sixteen(t), i2 * 128:(i2 + 1) * 128] = on[:, i2, :, hh * 128:(hh + 1) * 128]
            return 0

        lax.fori_loop(0, NT, norm, 0)

        for kh in range(2):
            def rows(ip, _):
                u = (jnp.dot(wot_ref[l], on_ref[kh, ip], preferred_element_type=F32) + cols_ref[l, :, 3:4]).astype(BF16)
                g = jax.nn.sigmoid(jnp.dot(wgt_ref[l], zn_ref[kh, ip], preferred_element_type=F32)
                                   + cols_ref[l, :, 4:5])
                out_ref[kh, ip] = (out_ref[kh, ip].astype(F32) + g * u.astype(F32)).astype(BF16)
                return 0

            lax.fori_loop(0, 8, rows, 0)

    prepare(0)
    g_pass(0)
    g_finish(0)
    for l in range(NL):
        for kh in range(2):
            outer(l, kh)
            project(l, kh)
        for h in range(NZ - 2):
            @pl.loop(0, 2 * NT)
            def _(n):
                arrive(l, h, n % NT, n // NT)
            if l == 0 and h == 0:
                g_pass(1)
                prepare(1)

        @pl.loop(0, NT)
        def _(t):
            arrive(l, NZ - 2, t, 0)

        @pl.loop(0, NT)
        def _(t):
            arrive(l, NZ - 2, t, 1)
            multiply(l, t)

        if l == 0:
            g_finish(1)
        drain(l)
        finish(l)


def solution(mesh):
    pair_spec = P(('batch', 'dap'), None, None)
    mask_spec = P(('batch', 'dap'), None)
    msa_spec = P(None, ('batch', 'dap'), None)
    vm = pl.BlockSpec(memory_space=pltpu.VMEM)
    dma = pltpu.SemaphoreType.DMA

    def bf(*shape):
        return pltpu.VMEM(shape, BF16)

    def f3(*shape):
        return pltpu.VMEM(shape, F32)

    call = pl.pallas_call(
        kernel,
        out_shape=jax.ShapeDtypeStruct((2, 8, 128, 256), BF16),
        in_specs=[vm] * 9 + [pl.BlockSpec(memory_space=pltpu.SMEM)],
        out_specs=vm,
        scratch_shapes=[
            bf(NL, 16, 256, 128), bf(8, 1024, 256),
            bf(NL, 128, 1024), bf(NL, NT, 4 * CC, 128), bf(NL, 128, 128), bf(NL, 128, 128),
            bf(2, 8, 128, 256), bf(256, 256),
            bf(NL, NT, 2, 256, 128), bf(NL, NT, 2, 256, 128), bf(NL, NZ, 2, NT, 2, 256, 128),
            f3(NL, 2, NT, 256, 128), f3(NL, NT, 256, 128), bf(256, 256), bf(2, 8, 128, 256),
            dma((NL, 8)), dma((NL, 8)), dma((NL, 8)), dma((NL, 8)), dma((NL,)),
            dma((NL, NT, 2)), dma((NL, NT, 2)),
            dma((NL, 2, NZ - 1, NT, 2)), dma((NL, 2, NZ - 1, NT, 2)),
            dma((NL, NZ, NT, 2)), dma((NL, NZ, NT, 2)),
            dma((NL, NT)), dma((NL, NT)),
        ],
        compiler_params=pltpu.CompilerParams(collective_id=0, has_side_effects=True),
        name='layers',
    )

    def device_fn(pair, mask, msa, opm_norm, opm_w_in, opm_b_in, opm_w_out, opm_b_out, tri_norm_in, tri_w_ab, tri_b_ab,
                  tri_w_gate, tri_b_gate, tri_norm_out, tri_w_out, tri_b_out):
        x = msa.astype(F32)
        xc = x - jnp.mean(x, axis=-1, keepdims=True)
        var = jnp.mean(xc * xc, axis=-1, keepdims=True)
        xh = xc * lax.rsqrt(var + EPS)
        nw = opm_norm.astype(F32)
        mn = (xh[None] * nw[:, 0][:, None, None] + nw[:, 1][:, None, None]).astype(BF16)
        bias = opm_b_in.astype(F32)
        b = (jnp.einsum('lmd,lsjm->ldjs', opm_w_in[:, :, 1], mn, preferred_element_type=F32)
             + bias[:, 1][:, :, None, None]).astype(BF16)
        b = b.reshape(2, 16, 2, 16, 64).transpose(0, 1, 3, 2, 4).reshape(2, 16, 16, 128)
        a = (jnp.einsum('lmc,lsim->lics', opm_w_in[:, :, 0], mn, preferred_element_type=F32)
             + bias[:, 0][:, None, :, None]).astype(BF16).reshape(2, 512, 64)
        al = jnp.concatenate([jnp.pad(a, ((0, 0), (0, 0), (0, 64))), jnp.pad(a, ((0, 0), (0, 0), (64, 0)))], axis=1)

        cols = jnp.concatenate([jnp.stack([opm_b_out, tri_norm_in[:, 0], tri_norm_in[:, 1], tri_b_out, tri_b_gate], axis=1),
                                tri_b_ab], axis=1).transpose(0, 2, 1).astype(F32)
        zt = pair.reshape(8, 2, 4, 2, 32, 128).transpose(3, 0, 5, 1, 2, 4).reshape(2, 8, 128, 256)
        mf = mask.reshape(8, 2, 4, 2, 32).transpose(3, 0, 1, 2, 4).reshape(2, 8, 1, 256).astype(F32)
        zt = call(zt, mf, al, b, opm_w_out, tri_w_ab.reshape(2, 128, 512), tri_w_gate, tri_w_out, cols,
                  tri_norm_out.astype(F32))
        return zt.reshape(2, 8, 128, 2, 4, 32).transpose(1, 3, 4, 0, 5, 2).reshape(16, 256, 128)

    return jax.shard_map(device_fn, mesh=mesh, in_specs=(pair_spec, mask_spec, msa_spec) + (P(),) * 13,
                         out_specs=pair_spec, check_vma=False)
```

```python
import jax
import jax.numpy as jnp
from jax import lax
from jax.sharding import PartitionSpec as P
from jax.experimental import pallas as pl
from jax.experimental.pallas import tpu as pltpu

EPS = 1e-5
MESH = pl.DeviceIdType.MESH
F32, BF16 = jnp.float32, jnp.bfloat16
NL = 2
NT = 8
CC = 16
TG = 2
NG = NT // TG
NZ = 4

NTD = (((1,), (1,)), ((), ()))


def place():
    me = lax.axis_index('dap')
    return me // 4, (me // 2) % 2, me % 2


def dap_of(z, y, c):
    return (z * 2 + y) * 2 + c


def sixteen(i):
    return pl.ds(pl.multiple_of(i * 16, 16), 16)


def kernel(zt_ref, maskin_ref, al_ref, bown_ref, wq_ref, wab_ref, wg_ref, wo_ref,
           bq_ref, ni_ref, bo_ref, bgate_ref, bab_ref, nout_ref,
           out_ref,
           cols_ref, no_ref, mask_ref, bg_ref, q_ref, wqt_ref, wabt_ref, wgt_ref, wot_ref, zn_ref, st_ref, aown_ref, arecv_ref, b_ref,
           obuf_ref, osend_ref, ost_ref, on_ref,
           sgi, rgi, sgd, rgd, sown, sa, ra, sz, rz, sd, rd, so, ro):
    z, y, c = place()
    chip = z * 2 + y
    ypart = dap_of(z, 1 - y, c)
    cpart = dap_of(z, y, 1 - c)

    bar = pltpu.get_barrier_semaphore()
    for r in range(1, 8):
        pl.semaphore_signal(bar, inc=1, device_id={'dap': lax.rem(chip + r, 8) * 2 + c}, device_id_type=MESH)
    pl.semaphore_signal(bar, inc=1, device_id={'dap': cpart}, device_id_type=MESH)
    pl.semaphore_wait(bar, 8)

    def bslot(l, ch, core):
        return bg_ref.at[l, :, sixteen((ch % 2 * 4 + ch // 2) * 2 + core), :]

    def g_ici(l, r):
        return pltpu.make_async_remote_copy(
            bown_ref.at[l], bslot(l, chip, c), sgi.at[l, r], rgi.at[l, r],
            device_id={'dap': lax.rem(chip + r, 8) * 2 + c}, device_id_type=MESH)

    def g_d2d(l, r):
        src = lax.rem(chip - r + 8, 8)
        return pltpu.make_async_remote_copy(
            bown_ref.at[l] if r == 0 else bslot(l, src, c), bslot(l, src, c), sgd.at[l, r], rgd.at[l, r],
            device_id={'dap': cpart}, device_id_type=MESH)

    def g_own(l):
        return pltpu.make_async_copy(bown_ref.at[l], bslot(l, chip, c), sown.at[l])

    def g_pass(l):
        for r in range(1, 8):
            g_ici(l, r).wait_recv()
            g_d2d(l, r).start()

    def g_finish(l):
        g_own(l).wait()
        for r in range(8):
            g_d2d(l, r).wait()
        for r in range(1, 8):
            g_ici(l, r).wait_send()

    def grp(g):
        return pl.ds(g * TG, TG)

    def cp_a(l, g, kh):
        return pltpu.make_async_remote_copy(aown_ref.at[l, kh, grp(g)], arecv_ref.at[l, kh, grp(g)], sa.at[l, g, kh],
                                            ra.at[l, g, kh], device_id={'dap': ypart}, device_id_type=MESH)

    def cp_o(l, t):
        return pltpu.make_async_remote_copy(osend_ref.at[l, t], obuf_ref.at[l, y, t], so.at[l, t], ro.at[l, t],
                                            device_id={'dap': ypart}, device_id_type=MESH)

    def cp_d(l, zs, g, kh, core):
        blk = b_ref.at[l, zs, core, kh, grp(g)]
        return pltpu.make_async_remote_copy(blk, blk, sd.at[l, zs, g, kh], rd.at[l, zs, g, kh],
                                            device_id={'dap': cpart}, device_id_type=MESH)

    def cp_z(l, up, h, g, kh, zs, dev):
        blk = b_ref.at[l, zs, c, kh, grp(g)]
        return pltpu.make_async_remote_copy(blk, blk, sz.at[l, int(up), h, g, kh], rz.at[l, int(up), h, g, kh],
                                            device_id={'dap': dev}, device_id_type=MESH)

    def send_z(l, up, h, g, kh):
        zs, zd = (z - h, z + 1) if up else (z + h, z - 1)
        return cp_z(l, up, h, g, kh, zs, dap_of(zd, y, c))

    def can_send(up, h):
        return (z - h >= 0) & (z + 1 < NZ) if up else (z + h < NZ) & (z - 1 >= 0)

    def can_recv(up, h):
        return z - h - 1 >= 0 if up else z + h + 1 < NZ

    def arrive(l, h, g, kh):
        for up in (False, True):
            @pl.when(can_recv(up, h))
            def _():
                zs = z - h - 1 if up else z + h + 1
                cp_z(l, up, h, g, kh, zs, cpart).wait_recv()
                if h < NZ - 2:
                    @pl.when(can_send(up, h + 1))
                    def _():
                        send_z(l, up, h + 1, g, kh).start()
                cp_d(l, zs, g, kh, c).start()

    def g_start(l):
        for r in range(1, 8):
            g_ici(l, r).start()
        g_d2d(l, 0).start()
        g_own(l).start()

    g_start(0)

    r_i = lax.broadcasted_iota(jnp.int32, (256, 256), 0)
    c_i = lax.broadcasted_iota(jnp.int32, (256, 256), 1)
    perm = ((r_i // 16 == c_i % 16) & (r_i % 16 == c_i // 16)).astype(F32).astype(BF16)

    def turn(w):
        return w.astype(F32).T.astype(BF16)

    def prepare(l):
        rows = [bq_ref[l:l + 1, :], ni_ref[l, 0:1, :], ni_ref[l, 1:2, :], bo_ref[l:l + 1, :], bgate_ref[l:l + 1, :]]
        rows = rows + [bab_ref[l, qq:qq + 1, :] for qq in range(4)]
        rows = [v.astype(F32) for v in rows] + [jnp.zeros((7, 128), F32)]
        cols_ref[l] = jnp.concatenate(rows, axis=0).T
        for n in range(2):
            no_ref[l, n] = jnp.broadcast_to(nout_ref[l, n:n + 1, :].astype(F32), (128, 128)).T

        @pl.loop(0, 4)
        def _(blk):
            r2 = lax.broadcasted_iota(jnp.int32, (256, 1024), 0)
            k2 = lax.broadcasted_iota(jnp.int32, (256, 1024), 1)
            sel = ((k2 // 32 == r2 % 32) & (k2 % 32 == r2 // 32 + blk * 8)).astype(F32).astype(BF16)
            w = jnp.dot(sel, wq_ref[l], preferred_element_type=F32)
            wqt_ref[l, :, pl.ds(pl.multiple_of(blk * 256, 256), 256)] = w.T.astype(BF16)
        for qq in range(4):
            w = turn(wab_ref[l, :, qq * 128:(qq + 1) * 128])
            wabt_ref[l, :, qq * CC:(qq + 1) * CC, :] = w.reshape(NT, CC, 128)
        wgt_ref[l] = turn(wg_ref[l])
        wot_ref[l] = turn(wo_ref[l])

    def outer(l, kh):
        @pl.loop(0, 8)
        def _(dpp):
            half = pl.ds(kh * 128, 128)
            bt = jnp.concatenate([bg_ref[l, dpp * 2, half, :], bg_ref[l, dpp * 2 + 1, half, :]], axis=0)
            for par in range(2):
                for h in range(2):
                    rows = lax.dot_general(al_ref[l, pl.ds(par * 512 + h * 256, 256), :], bt, NTD,
                                           preferred_element_type=F32)
                    rows = (rows * (1.0 / 64)).astype(BF16).reshape(4, 2, 32, 256)
                    for e in range(2):
                        at = pl.ds(pl.multiple_of((dpp * 4 + e * 2 + par) * 32, 32), 32)
                        for i2 in range(2):
                            q_ref[pl.ds(h * 4, 4), at, i2 * 128:(i2 + 1) * 128] = rows[:, i2, :, e * 128:(e + 1) * 128]

        src = zt_ref if l == 0 else out_ref

        def rows(ip, _):
            upd = jnp.dot(wqt_ref[l], q_ref[ip], preferred_element_type=F32) + cols_ref[l, :, 0:1]
            zi = (src[kh, ip].astype(F32) + upd.astype(BF16).astype(F32)).astype(BF16)
            out_ref[kh, ip] = zi
            x = zi.astype(F32)
            xc = x - jnp.mean(x, axis=0, keepdims=True)
            var = jnp.mean(xc * xc, axis=0, keepdims=True)
            zn_ref[kh, ip] = (xc * lax.rsqrt(var + EPS) * cols_ref[l, :, 1:2] + cols_ref[l, :, 2:3]).astype(BF16)
            return 0

        lax.fori_loop(0, 8, rows, 0)

    def project(l, kh):
        def chunk(t, _):
            bias = jnp.concatenate([jnp.broadcast_to(cols_ref[l, sixteen(t), 5 + qq:6 + qq], (CC, 256))
                                    for qq in range(4)], axis=0)
            w = wabt_ref[l, t]

            def rows(ip, _):
                p = jnp.dot(w, zn_ref[kh, ip], preferred_element_type=F32) + bias
                m = mask_ref[kh, ip]
                at = (m * jax.nn.sigmoid(p[16:32]) * p[0:16]).astype(BF16)
                bt = (m * jax.nn.sigmoid(p[48:64]) * p[32:48]).astype(BF16)
                for i2 in range(2):
                    ln = slice(i2 * 128, (i2 + 1) * 128)
                    st_ref[sixteen(ip * 2 + i2), 0:128] = at[:, ln]
                    st_ref[sixteen(ip * 2 + i2), 128:256] = bt[:, ln]
                return 0

            lax.fori_loop(0, 8, rows, 0, unroll=4)
            ab = jnp.dot(perm, st_ref[...], preferred_element_type=F32).astype(BF16)
            aown_ref[l, kh, t] = ab[:, 0:128]
            b_ref[l, z, c, kh, t] = ab[:, 128:256]
            return 0

        @pl.loop(0, NG)
        def _(g):
            lax.fori_loop(g * TG, g * TG + TG, chunk, 0)
            for up in (False, True):
                @pl.when(can_send(up, 0))
                def _():
                    send_z(l, up, 0, g, kh).start()
            cp_a(l, g, kh).start()
            cp_d(l, z, g, kh, c).start()

    def ready(l, g):
        for kh in range(2):
            cp_a(l, g, kh).wait_recv()
            for zs in range(NZ):
                cp_d(l, zs, g, kh, 1 - c).wait_recv()

    def multiply(l, t):
        for cc in range(CC):
            rs = pl.ds(cc * 16, 16)
            lhs = jnp.concatenate([jnp.concatenate([r[l, kh, t, rs, :] for kh in range(2)], axis=1)
                                   for r in (aown_ref, arecv_ref)], axis=0)
            rhs = jnp.concatenate([jnp.concatenate([b_ref[l, zs, k, kh, t, rs, :] for kh in range(2)], axis=1)
                                   for zs in range(NZ) for k in range(2)], axis=0)
            o = lax.dot_general(lhs, rhs, NTD, preferred_element_type=F32)
            obuf_ref[l, y, t, rs, :] = o[0:16]
            osend_ref[l, t, rs, :] = o[16:32]
        cp_o(l, t).start()

    def drain(l):
        @pl.loop(0, NT)
        def _(t):
            cp_o(l, t).wait()

        @pl.loop(0, NG)
        def _(g):
            for kh in range(2):
                cp_a(l, g, kh).wait_send()
                for zs in range(NZ):
                    cp_d(l, zs, g, kh, c).wait_send()
                for up in (False, True):
                    for h in range(NZ - 1):
                        @pl.when(can_send(up, h))
                        def _():
                            send_z(l, up, h, g, kh).wait_send()

    def finish(l):
        def load(t, cc, hh):
            return obuf_ref[l, hh, t, pl.ds(cc * 16, 16), :]

        zero = jnp.zeros((16, 128), F32)

        def add1(t, s):
            for cc in range(CC):
                s = tuple(s[hh] + load(t, cc, hh) for hh in range(2))
            return s

        tot = lax.fori_loop(0, NT, add1, (zero, zero))
        mean = tuple(s * (1.0 / 128) for s in tot)

        def add2(t, s):
            for cc in range(CC):
                d = tuple(load(t, cc, hh) - mean[hh] for hh in range(2))
                s = tuple(s[hh] + d[hh] * d[hh] for hh in range(2))
            return s

        sq = lax.fori_loop(0, NT, add2, (zero, zero))
        inv = tuple(lax.rsqrt(s * (1.0 / 128) + EPS) for s in sq)

        def norm(t, _):
            for cc in range(CC):
                for hh in range(2):
                    one = pl.ds(t * CC + cc, 1)
                    v = (load(t, cc, hh) - mean[hh]) * inv[hh] * no_ref[l, 0, one, :] + no_ref[l, 1, one, :]
                    ost_ref[pl.ds(cc * 16, 16), pl.ds(hh * 128, 128)] = v.astype(BF16)
            on = jnp.dot(perm, ost_ref[...], preferred_element_type=F32).astype(BF16).reshape(8, 2, CC, 256)
            for hh in range(2):
                for i2 in range(2):
                    on_ref[hh, :, sixteen(t), i2 * 128:(i2 + 1) * 128] = on[:, i2, :, hh * 128:(hh + 1) * 128]
            return 0

        lax.fori_loop(0, NT, norm, 0)

        for kh in range(2):
            def rows(ip, _):
                u = (jnp.dot(wot_ref[l], on_ref[kh, ip], preferred_element_type=F32) + cols_ref[l, :, 3:4]).astype(BF16)
                g = jax.nn.sigmoid(jnp.dot(wgt_ref[l], zn_ref[kh, ip], preferred_element_type=F32)
                                   + cols_ref[l, :, 4:5])
                out_ref[kh, ip] = (out_ref[kh, ip].astype(F32) + g * u.astype(F32)).astype(BF16)
                return 0

            lax.fori_loop(0, 8, rows, 0)

    prepare(0)
    m = maskin_ref[...].astype(F32)
    for kh in range(2):
        half = jnp.concatenate([m[:, zz * 64 + kh * 32:zz * 64 + kh * 32 + 32] for zz in range(NZ)], axis=1)
        for i in range(16):
            mask_ref[kh, i // 2, :, i % 2 * 128:(i % 2 + 1) * 128] = half[i:i + 1, :]
    g_pass(0)
    g_finish(0)
    for l in range(NL):
        for kh in range(2):
            outer(l, kh)
            project(l, kh)
        for h in range(NZ - 2):
            @pl.loop(0, 2 * NG)
            def _(n):
                arrive(l, h, n % NG, n // NG)
            if l == 0 and h == 0:
                prepare(1)
        if l == 0:
            g_start(1)

        @pl.loop(0, NG)
        def _(g):
            arrive(l, NZ - 2, g, 0)

        @pl.loop(0, NG)
        def _(g):
            arrive(l, NZ - 2, g, 1)
            ready(l, g)

            @pl.loop(0, TG)
            def _(k):
                multiply(l, g * TG + k)

        if l == 0:
            g_pass(1)
        drain(l)
        finish(l)
        if l == 0:
            g_finish(1)


def solution(mesh):
    pair_spec = P(('batch', 'dap'), None, None)
    mask_spec = P(('batch', 'dap'), None)
    msa_spec = P(None, ('batch', 'dap'), None)
    vm = pl.BlockSpec(memory_space=pltpu.VMEM)
    dma = pltpu.SemaphoreType.DMA

    def bf(*shape):
        return pltpu.VMEM(shape, BF16)

    def f3(*shape):
        return pltpu.VMEM(shape, F32)

    call = pl.pallas_call(
        kernel,
        out_shape=jax.ShapeDtypeStruct((2, 8, 128, 256), BF16),
        in_specs=[vm] * 14,
        out_specs=vm,
        scratch_shapes=[
            f3(NL, 128, 16), f3(NL, 2, 128, 128), f3(2, 8, 1, 256),
            bf(NL, 16, 256, 128), bf(8, 1024, 256),
            bf(NL, 128, 1024), bf(NL, NT, 4 * CC, 128), bf(NL, 128, 128), bf(NL, 128, 128),
            bf(2, 8, 128, 256), bf(256, 256),
            bf(NL, 2, NT, 256, 128), bf(NL, 2, NT, 256, 128), bf(NL, NZ, 2, 2, NT, 256, 128),
            f3(NL, 2, NT, 256, 128), f3(NL, NT, 256, 128), bf(256, 256), bf(2, 8, 128, 256),
            dma((NL, 8)), dma((NL, 8)), dma((NL, 8)), dma((NL, 8)), dma((NL,)),
            dma((NL, NG, 2)), dma((NL, NG, 2)),
            dma((NL, 2, NZ - 1, NG, 2)), dma((NL, 2, NZ - 1, NG, 2)),
            dma((NL, NZ, NG, 2)), dma((NL, NZ, NG, 2)),
            dma((NL, NT)), dma((NL, NT)),
        ],
        compiler_params=pltpu.CompilerParams(collective_id=0, has_side_effects=True),
        name='layers',
    )

    def device_fn(pair, mask, msa, opm_norm, opm_w_in, opm_b_in, opm_w_out, opm_b_out, tri_norm_in, tri_w_ab, tri_b_ab,
                  tri_w_gate, tri_b_gate, tri_norm_out, tri_w_out, tri_b_out):
        x = msa.astype(F32)
        xc = x - jnp.mean(x, axis=-1, keepdims=True)
        var = jnp.mean(xc * xc, axis=-1, keepdims=True)
        xh = xc * lax.rsqrt(var + EPS)
        nw = opm_norm.astype(F32)
        mn = (xh[None] * nw[:, 0][:, None, None] + nw[:, 1][:, None, None]).astype(BF16)
        bias = opm_b_in.astype(F32)
        b = (jnp.einsum('lmd,lsjm->ldjs', opm_w_in[:, :, 1], mn, preferred_element_type=F32)
             + bias[:, 1][:, :, None, None]).astype(BF16)
        b = b.reshape(2, 16, 2, 16, 64).transpose(0, 1, 3, 2, 4).reshape(2, 16, 16, 128)
        a = (jnp.einsum('lmc,lsim->lics', opm_w_in[:, :, 0], mn, preferred_element_type=F32)
             + bias[:, 0][:, None, :, None]).astype(BF16).reshape(2, 512, 64)
        al = jnp.concatenate([jnp.pad(a, ((0, 0), (0, 0), (0, 64))), jnp.pad(a, ((0, 0), (0, 0), (64, 0)))], axis=1)

        zt = pair.reshape(8, 2, 4, 2, 32, 128).transpose(3, 0, 5, 1, 2, 4).reshape(2, 8, 128, 256)
        zt = call(zt, mask, al, b, opm_w_out, tri_w_ab.reshape(2, 128, 512), tri_w_gate, tri_w_out,
                  opm_b_out, tri_norm_in, tri_b_out, tri_b_gate, tri_b_ab, tri_norm_out)
        return zt.reshape(2, 8, 128, 2, 4, 32).transpose(1, 3, 4, 0, 5, 2).reshape(16, 256, 128)

    return jax.shard_map(device_fn, mesh=mesh, in_specs=(pair_spec, mask_spec, msa_spec) + (P(),) * 13,
                         out_specs=pair_spec, check_vma=False)
```

```python
import jax
import jax.numpy as jnp
from jax import lax
from jax.sharding import PartitionSpec as P
from jax.experimental import pallas as pl
from jax.experimental.pallas import tpu as pltpu

EPS = 1e-5
MESH = pl.DeviceIdType.MESH
F32, BF16 = jnp.float32, jnp.bfloat16
NL = 2
NT = 8
CC = 16
TG = 1
NG = NT // TG
NZ = 4

NTD = (((1,), (1,)), ((), ()))


def place():
    me = lax.axis_index('dap')
    return me // 4, (me // 2) % 2, me % 2


def dap_of(z, y, c):
    return (z * 2 + y) * 2 + c


def sixteen(i):
    return pl.ds(pl.multiple_of(i * 16, 16), 16)


def kernel(zt_ref, maskin_ref, al_ref, bown_ref, wq_ref, wab_ref, wg_ref, wo_ref,
           bq_ref, ni_ref, bo_ref, bgate_ref, bab_ref, nout_ref,
           out_ref,
           cols_ref, no_ref, mask_ref, bg_ref, q_ref, wqt_ref, wabt_ref, wgt_ref, wot_ref, zn_ref, st_ref, aown_ref, arecv_ref, b_ref,
           obuf_ref, osend_ref, ost_ref, on_ref,
           sgi, rgi, sgd, rgd, sown, sa, ra, sz, rz, sd, rd, so, ro):
    z, y, c = place()
    chip = z * 2 + y
    ypart = dap_of(z, 1 - y, c)
    cpart = dap_of(z, y, 1 - c)

    bar = pltpu.get_barrier_semaphore()
    for r in range(1, 8):
        pl.semaphore_signal(bar, inc=1, device_id={'dap': lax.rem(chip + r, 8) * 2 + c}, device_id_type=MESH)
    pl.semaphore_signal(bar, inc=1, device_id={'dap': cpart}, device_id_type=MESH)
    pl.semaphore_wait(bar, 8)

    def bslot(l, ch, core):
        return bg_ref.at[l, :, sixteen((ch % 2 * 4 + ch // 2) * 2 + core), :]

    def g_ici(l, r):
        return pltpu.make_async_remote_copy(
            bown_ref.at[l], bslot(l, chip, c), sgi.at[l, r], rgi.at[l, r],
            device_id={'dap': lax.rem(chip + r, 8) * 2 + c}, device_id_type=MESH)

    def g_d2d(l, r):
        src = lax.rem(chip - r + 8, 8)
        return pltpu.make_async_remote_copy(
            bown_ref.at[l] if r == 0 else bslot(l, src, c), bslot(l, src, c), sgd.at[l, r], rgd.at[l, r],
            device_id={'dap': cpart}, device_id_type=MESH)

    def g_own(l):
        return pltpu.make_async_copy(bown_ref.at[l], bslot(l, chip, c), sown.at[l])

    def g_pass(l):
        for r in range(1, 8):
            g_ici(l, r).wait_recv()
            g_d2d(l, r).start()

    def g_finish(l):
        g_own(l).wait()
        for r in range(8):
            g_d2d(l, r).wait()
        for r in range(1, 8):
            g_ici(l, r).wait_send()

    def grp(g):
        return pl.ds(g * TG, TG)

    def cp_a(l, g, kh):
        return pltpu.make_async_remote_copy(aown_ref.at[l, kh, grp(g)], arecv_ref.at[l, kh, grp(g)], sa.at[l, g, kh],
                                            ra.at[l, g, kh], device_id={'dap': ypart}, device_id_type=MESH)

    def cp_o(l, t):
        return pltpu.make_async_remote_copy(osend_ref.at[l, t], obuf_ref.at[l, y, t], so.at[l, t], ro.at[l, t],
                                            device_id={'dap': ypart}, device_id_type=MESH)

    def cp_d(l, zs, g, kh, core):
        blk = b_ref.at[l, zs, core, kh, grp(g)]
        return pltpu.make_async_remote_copy(blk, blk, sd.at[l, zs, g, kh], rd.at[l, zs, g, kh],
                                            device_id={'dap': cpart}, device_id_type=MESH)

    def cp_z(l, up, h, g, kh, zs, dev):
        blk = b_ref.at[l, zs, c, kh, grp(g)]
        return pltpu.make_async_remote_copy(blk, blk, sz.at[l, int(up), h, g, kh], rz.at[l, int(up), h, g, kh],
                                            device_id={'dap': dev}, device_id_type=MESH)

    def send_z(l, up, h, g, kh):
        zs, zd = (z - h, z + 1) if up else (z + h, z - 1)
        return cp_z(l, up, h, g, kh, zs, dap_of(zd, y, c))

    def can_send(up, h):
        return (z - h >= 0) & (z + 1 < NZ) if up else (z + h < NZ) & (z - 1 >= 0)

    def can_recv(up, h):
        return z - h - 1 >= 0 if up else z + h + 1 < NZ

    def arrive(l, h, g, kh):
        for up in (False, True):
            @pl.when(can_recv(up, h))
            def _():
                zs = z - h - 1 if up else z + h + 1
                cp_z(l, up, h, g, kh, zs, cpart).wait_recv()
                cp_d(l, zs, g, kh, c).start()

    def forward(l, h, g):
        for up in (False, True):
            @pl.when(can_send(up, h + 1))
            def _():
                for kh in range(2):
                    send_z(l, up, h + 1, g, kh).start()

    def g_start(l):
        for r in range(1, 8):
            g_ici(l, r).start()
        g_d2d(l, 0).start()
        g_own(l).start()

    g_start(0)

    r_i = lax.broadcasted_iota(jnp.int32, (256, 256), 0)
    c_i = lax.broadcasted_iota(jnp.int32, (256, 256), 1)
    perm = ((r_i // 16 == c_i % 16) & (r_i % 16 == c_i // 16)).astype(F32).astype(BF16)

    def turn(w):
        return w.astype(F32).T.astype(BF16)

    def prepare(l):
        rows = [bq_ref[l:l + 1, :], ni_ref[l, 0:1, :], ni_ref[l, 1:2, :], bo_ref[l:l + 1, :], bgate_ref[l:l + 1, :]]
        rows = rows + [bab_ref[l, qq:qq + 1, :] for qq in range(4)]
        rows = [v.astype(F32) for v in rows] + [jnp.zeros((7, 128), F32)]
        cols_ref[l] = jnp.concatenate(rows, axis=0).T
        for n in range(2):
            no_ref[l, n] = jnp.broadcast_to(nout_ref[l, n:n + 1, :].astype(F32), (128, 128)).T

        @pl.loop(0, 4)
        def _(blk):
            r2 = lax.broadcasted_iota(jnp.int32, (256, 1024), 0)
            k2 = lax.broadcasted_iota(jnp.int32, (256, 1024), 1)
            sel = ((k2 // 32 == r2 % 32) & (k2 % 32 == r2 // 32 + blk * 8)).astype(F32).astype(BF16)
            w = jnp.dot(sel, wq_ref[l], preferred_element_type=F32)
            wqt_ref[l, :, pl.ds(pl.multiple_of(blk * 256, 256), 256)] = w.T.astype(BF16)
        for qq in range(4):
            w = turn(wab_ref[l, :, qq * 128:(qq + 1) * 128])
            wabt_ref[l, :, qq * CC:(qq + 1) * CC, :] = w.reshape(NT, CC, 128)
        wgt_ref[l] = turn(wg_ref[l])
        wot_ref[l] = turn(wo_ref[l])

    def outer(l, kh):
        @pl.loop(0, 8)
        def _(dpp):
            half = pl.ds(kh * 128, 128)
            bt = jnp.concatenate([bg_ref[l, dpp * 2, half, :], bg_ref[l, dpp * 2 + 1, half, :]], axis=0)
            for par in range(2):
                for h in range(2):
                    rows = lax.dot_general(al_ref[l, pl.ds(par * 512 + h * 256, 256), :], bt, NTD,
                                           preferred_element_type=F32)
                    rows = (rows * (1.0 / 64)).astype(BF16).reshape(4, 2, 32, 256)
                    for e in range(2):
                        at = pl.ds(pl.multiple_of((dpp * 4 + e * 2 + par) * 32, 32), 32)
                        for i2 in range(2):
                            q_ref[pl.ds(h * 4, 4), at, i2 * 128:(i2 + 1) * 128] = rows[:, i2, :, e * 128:(e + 1) * 128]

        src = zt_ref if l == 0 else out_ref

        def rows(ip, _):
            upd = jnp.dot(wqt_ref[l], q_ref[ip], preferred_element_type=F32) + cols_ref[l, :, 0:1]
            zi = (src[kh, ip].astype(F32) + upd.astype(BF16).astype(F32)).astype(BF16)
            out_ref[kh, ip] = zi
            x = zi.astype(F32)
            xc = x - jnp.mean(x, axis=0, keepdims=True)
            var = jnp.mean(xc * xc, axis=0, keepdims=True)
            zn_ref[kh, ip] = (xc * lax.rsqrt(var + EPS) * cols_ref[l, :, 1:2] + cols_ref[l, :, 2:3]).astype(BF16)
            return 0

        lax.fori_loop(0, 8, rows, 0)

    def project(l, kh):
        def chunk(t, _):
            bias = jnp.concatenate([jnp.broadcast_to(cols_ref[l, sixteen(t), 5 + qq:6 + qq], (CC, 256))
                                    for qq in range(4)], axis=0)
            w = wabt_ref[l, t]

            def rows(ip, _):
                p = jnp.dot(w, zn_ref[kh, ip], preferred_element_type=F32) + bias
                m = mask_ref[kh, ip]
                at = (m * jax.nn.sigmoid(p[16:32]) * p[0:16]).astype(BF16)
                bt = (m * jax.nn.sigmoid(p[48:64]) * p[32:48]).astype(BF16)
                for i2 in range(2):
                    ln = slice(i2 * 128, (i2 + 1) * 128)
                    st_ref[sixteen(ip * 2 + i2), 0:128] = at[:, ln]
                    st_ref[sixteen(ip * 2 + i2), 128:256] = bt[:, ln]
                return 0

            lax.fori_loop(0, 8, rows, 0, unroll=4)
            ab = jnp.dot(perm, st_ref[...], preferred_element_type=F32).astype(BF16)
            aown_ref[l, kh, t] = ab[:, 0:128]
            b_ref[l, z, c, kh, t] = ab[:, 128:256]
            return 0

        @pl.loop(0, NG)
        def _(g):
            lax.fori_loop(g * TG, g * TG + TG, chunk, 0)
            for up in (False, True):
                @pl.when(can_send(up, 0))
                def _():
                    send_z(l, up, 0, g, kh).start()
            cp_a(l, g, kh).start()
            cp_d(l, z, g, kh, c).start()

    def ready(l, g):
        for kh in range(2):
            cp_a(l, g, kh).wait_recv()
            for zs in range(NZ):
                cp_d(l, zs, g, kh, 1 - c).wait_recv()

    def multiply(l, t):
        for cc in range(CC):
            rs = pl.ds(cc * 16, 16)
            lhs = jnp.concatenate([jnp.concatenate([r[l, kh, t, rs, :] for kh in range(2)], axis=1)
                                   for r in (aown_ref, arecv_ref)], axis=0)
            rhs = jnp.concatenate([jnp.concatenate([b_ref[l, zs, k, kh, t, rs, :] for kh in range(2)], axis=1)
                                   for zs in range(NZ) for k in range(2)], axis=0)
            o = lax.dot_general(lhs, rhs, NTD, preferred_element_type=F32)
            obuf_ref[l, y, t, rs, :] = o[0:16]
            osend_ref[l, t, rs, :] = o[16:32]
        cp_o(l, t).start()

    def drain(l):
        @pl.loop(0, NT)
        def _(t):
            cp_o(l, t).wait()

        @pl.loop(0, NG)
        def _(g):
            for kh in range(2):
                cp_a(l, g, kh).wait_send()
                for zs in range(NZ):
                    cp_d(l, zs, g, kh, c).wait_send()
                for up in (False, True):
                    for h in range(NZ - 1):
                        @pl.when(can_send(up, h))
                        def _():
                            send_z(l, up, h, g, kh).wait_send()

    def finish(l):
        def load(t, cc, hh):
            return obuf_ref[l, hh, t, pl.ds(cc * 16, 16), :]

        zero = jnp.zeros((16, 128), F32)

        def add1(t, s):
            for cc in range(CC):
                s = tuple(s[hh] + load(t, cc, hh) for hh in range(2))
            return s

        tot = lax.fori_loop(0, NT, add1, (zero, zero))
        mean = tuple(s * (1.0 / 128) for s in tot)

        def add2(t, s):
            for cc in range(CC):
                d = tuple(load(t, cc, hh) - mean[hh] for hh in range(2))
                s = tuple(s[hh] + d[hh] * d[hh] for hh in range(2))
            return s

        sq = lax.fori_loop(0, NT, add2, (zero, zero))
        inv = tuple(lax.rsqrt(s * (1.0 / 128) + EPS) for s in sq)

        def norm(t, _):
            for cc in range(CC):
                for hh in range(2):
                    one = pl.ds(t * CC + cc, 1)
                    v = (load(t, cc, hh) - mean[hh]) * inv[hh] * no_ref[l, 0, one, :] + no_ref[l, 1, one, :]
                    ost_ref[pl.ds(cc * 16, 16), pl.ds(hh * 128, 128)] = v.astype(BF16)
            on = jnp.dot(perm, ost_ref[...], preferred_element_type=F32).astype(BF16).reshape(8, 2, CC, 256)
            for hh in range(2):
                for i2 in range(2):
                    on_ref[hh, :, sixteen(t), i2 * 128:(i2 + 1) * 128] = on[:, i2, :, hh * 128:(hh + 1) * 128]
            return 0

        lax.fori_loop(0, NT, norm, 0)

        for kh in range(2):
            def rows(ip, _):
                u = (jnp.dot(wot_ref[l], on_ref[kh, ip], preferred_element_type=F32) + cols_ref[l, :, 3:4]).astype(BF16)
                g = jax.nn.sigmoid(jnp.dot(wgt_ref[l], zn_ref[kh, ip], preferred_element_type=F32)
                                   + cols_ref[l, :, 4:5])
                out_ref[kh, ip] = (out_ref[kh, ip].astype(F32) + g * u.astype(F32)).astype(BF16)
                return 0

            lax.fori_loop(0, 8, rows, 0)

    prepare(0)
    m = maskin_ref[...].astype(F32)
    for kh in range(2):
        half = jnp.concatenate([m[:, zz * 64 + kh * 32:zz * 64 + kh * 32 + 32] for zz in range(NZ)], axis=1)
        for i in range(16):
            mask_ref[kh, i // 2, :, i % 2 * 128:(i % 2 + 1) * 128] = half[i:i + 1, :]
    g_pass(0)
    g_finish(0)
    for l in range(NL):
        for kh in range(2):
            outer(l, kh)
            project(l, kh)
        @pl.loop(0, NG)
        def _(g):
            arrive(l, 0, g, 0)

        @pl.loop(0, NG)
        def _(g):
            arrive(l, 0, g, 1)
            forward(l, 0, g)

        if l == 0:
            prepare(1)

        @pl.loop(0, NG)
        def _(g):
            for kh in range(2):
                arrive(l, 1, g, kh)
            forward(l, 1, g)

        if l == 0:
            g_start(1)

        @pl.loop(0, NG)
        def _(g):
            for kh in range(2):
                arrive(l, 2, g, kh)
            ready(l, g)

            @pl.loop(0, TG)
            def _(k):
                multiply(l, g * TG + k)

        if l == 0:
            g_pass(1)
        drain(l)
        finish(l)
        if l == 0:
            g_finish(1)


def solution(mesh):
    pair_spec = P(('batch', 'dap'), None, None)
    mask_spec = P(('batch', 'dap'), None)
    msa_spec = P(None, ('batch', 'dap'), None)
    vm = pl.BlockSpec(memory_space=pltpu.VMEM)
    dma = pltpu.SemaphoreType.DMA

    def bf(*shape):
        return pltpu.VMEM(shape, BF16)

    def f3(*shape):
        return pltpu.VMEM(shape, F32)

    call = pl.pallas_call(
        kernel,
        out_shape=jax.ShapeDtypeStruct((2, 8, 128, 256), BF16),
        in_specs=[vm] * 14,
        out_specs=vm,
        scratch_shapes=[
            f3(NL, 128, 16), f3(NL, 2, 128, 128), f3(2, 8, 1, 256),
            bf(NL, 16, 256, 128), bf(8, 1024, 256),
            bf(NL, 128, 1024), bf(NL, NT, 4 * CC, 128), bf(NL, 128, 128), bf(NL, 128, 128),
            bf(2, 8, 128, 256), bf(256, 256),
            bf(NL, 2, NT, 256, 128), bf(NL, 2, NT, 256, 128), bf(NL, NZ, 2, 2, NT, 256, 128),
            f3(NL, 2, NT, 256, 128), f3(NL, NT, 256, 128), bf(256, 256), bf(2, 8, 128, 256),
            dma((NL, 8)), dma((NL, 8)), dma((NL, 8)), dma((NL, 8)), dma((NL,)),
            dma((NL, NG, 2)), dma((NL, NG, 2)),
            dma((NL, 2, NZ - 1, NG, 2)), dma((NL, 2, NZ - 1, NG, 2)),
            dma((NL, NZ, NG, 2)), dma((NL, NZ, NG, 2)),
            dma((NL, NT)), dma((NL, NT)),
        ],
        compiler_params=pltpu.CompilerParams(collective_id=0, has_side_effects=True),
        name='layers',
    )

    def device_fn(pair, mask, msa, opm_norm, opm_w_in, opm_b_in, opm_w_out, opm_b_out, tri_norm_in, tri_w_ab, tri_b_ab,
                  tri_w_gate, tri_b_gate, tri_norm_out, tri_w_out, tri_b_out):
        x = msa.astype(F32)
        xc = x - jnp.mean(x, axis=-1, keepdims=True)
        var = jnp.mean(xc * xc, axis=-1, keepdims=True)
        xh = xc * lax.rsqrt(var + EPS)
        nw = opm_norm.astype(F32)
        mn = (xh[None] * nw[:, 0][:, None, None] + nw[:, 1][:, None, None]).astype(BF16)
        bias = opm_b_in.astype(F32)
        b = (jnp.einsum('lmd,lsjm->ldjs', opm_w_in[:, :, 1], mn, preferred_element_type=F32)
             + bias[:, 1][:, :, None, None]).astype(BF16)
        b = b.reshape(2, 16, 2, 16, 64).transpose(0, 1, 3, 2, 4).reshape(2, 16, 16, 128)
        a = (jnp.einsum('lmc,lsim->lics', opm_w_in[:, :, 0], mn, preferred_element_type=F32)
             + bias[:, 0][:, None, :, None]).astype(BF16).reshape(2, 512, 64)
        al = jnp.concatenate([jnp.pad(a, ((0, 0), (0, 0), (0, 64))), jnp.pad(a, ((0, 0), (0, 0), (64, 0)))], axis=1)

        zt = pair.reshape(8, 2, 4, 2, 32, 128).transpose(3, 0, 5, 1, 2, 4).reshape(2, 8, 128, 256)
        zt = call(zt, mask, al, b, opm_w_out, tri_w_ab.reshape(2, 128, 512), tri_w_gate, tri_w_out,
                  opm_b_out, tri_norm_in, tri_b_out, tri_b_gate, tri_b_ab, tri_norm_out)
        return zt.reshape(2, 8, 128, 2, 4, 32).transpose(1, 3, 4, 0, 5, 2).reshape(16, 256, 128)

    return jax.shard_map(device_fn, mesh=mesh, in_specs=(pair_spec, mask_spec, msa_spec) + (P(),) * 13,
                         out_specs=pair_spec, check_vma=False)
```

```python
import jax
import jax.numpy as jnp
from jax import lax
from jax.sharding import PartitionSpec as P
from jax.experimental import pallas as pl
from jax.experimental.pallas import tpu as pltpu

EPS = 1e-5
MESH = pl.DeviceIdType.MESH
F32, BF16 = jnp.float32, jnp.bfloat16
NL = 2
NT = 8
CC = 16
TG = 1
NG = NT // TG
NZ = 4

NTD = (((1,), (1,)), ((), ()))


def place():
    me = lax.axis_index('dap')
    return me // 4, (me // 2) % 2, me % 2


def dap_of(z, y, c):
    return (z * 2 + y) * 2 + c


def sixteen(i):
    return pl.ds(pl.multiple_of(i * 16, 16), 16)


def kernel(zt_ref, maskin_ref, al_ref, bown_ref, wq_ref, wab_ref, wg_ref, wo_ref,
           bq_ref, ni_ref, bo_ref, bgate_ref, bab_ref, nout_ref,
           out_ref,
           cols_ref, no_ref, mask_ref, bg_ref, q_ref, wqt_ref, wabt_ref, wgt_ref, wot_ref, zn_ref, st_ref, aown_ref, arecv_ref, b_ref,
           obuf_ref, osend_ref, ost_ref, on_ref,
           sgi, rgi, sgd, rgd, sown, sa, ra, sz, rz, sd, rd, so, ro):
    z, y, c = place()
    ypart = dap_of(z, 1 - y, c)
    cpart = dap_of(z, y, 1 - c)

    bar = pltpu.get_barrier_semaphore()
    for r in range(1, NZ):
        pl.semaphore_signal(bar, inc=1, device_id={'dap': dap_of(lax.rem(z + r, NZ), y, c)}, device_id_type=MESH)
    pl.semaphore_signal(bar, inc=1, device_id={'dap': ypart}, device_id_type=MESH)
    pl.semaphore_signal(bar, inc=1, device_id={'dap': cpart}, device_id_type=MESH)
    pl.semaphore_wait(bar, NZ + 1)

    def bslot(l, zz, yy, core):
        return bg_ref.at[l, :, sixteen((yy * NZ + zz) * 2 + core), :]

    def g_z(l, r):
        return pltpu.make_async_remote_copy(
            bown_ref.at[l], bslot(l, z, y, c), sgi.at[l, r], rgi.at[l, r],
            device_id={'dap': dap_of(lax.rem(z + r, NZ), y, c)}, device_id_type=MESH)

    def g_fwd(l, r, other):
        zs = lax.rem(z - r + NZ, NZ)
        src = bown_ref.at[l] if r == 0 else bslot(l, zs, y, c)
        if other == 0:
            return pltpu.make_async_remote_copy(src, bslot(l, zs, y, c), sgi.at[l, NZ + r], rgi.at[l, NZ + r],
                                                device_id={'dap': ypart}, device_id_type=MESH)
        if other == 1:
            return pltpu.make_async_remote_copy(src, bslot(l, zs, y, c), sgd.at[l, r], rgd.at[l, r],
                                                device_id={'dap': cpart}, device_id_type=MESH)
        far = bslot(l, zs, 1 - y, c)
        return pltpu.make_async_remote_copy(far, far, sgd.at[l, NZ + r], rgd.at[l, NZ + r],
                                            device_id={'dap': cpart}, device_id_type=MESH)

    def g_own(l):
        return pltpu.make_async_copy(bown_ref.at[l], bslot(l, z, y, c), sown.at[l])

    def g_pass_z(l):
        for r in range(1, NZ):
            g_z(l, r).wait_recv()
            g_fwd(l, r, 0).start()
            g_fwd(l, r, 1).start()

    def g_pass_y(l):
        for r in range(NZ):
            g_fwd(l, r, 0).wait_recv()
            g_fwd(l, r, 2).start()

    def g_finish(l):
        g_own(l).wait()
        for r in range(NZ):
            g_fwd(l, r, 1).wait()
            g_fwd(l, r, 2).wait()
            g_fwd(l, r, 0).wait_send()
            if r > 0:
                g_z(l, r).wait_send()

    def grp(g):
        return pl.ds(g * TG, TG)

    def cp_a(l, g, kh):
        return pltpu.make_async_remote_copy(aown_ref.at[l, kh, grp(g)], arecv_ref.at[l, kh, grp(g)], sa.at[l, g, kh],
                                            ra.at[l, g, kh], device_id={'dap': ypart}, device_id_type=MESH)

    def cp_o(l, t):
        return pltpu.make_async_remote_copy(osend_ref.at[l, t], obuf_ref.at[l, y, t], so.at[l, t], ro.at[l, t],
                                            device_id={'dap': ypart}, device_id_type=MESH)

    def cp_d(l, zs, g, kh, core):
        blk = b_ref.at[l, zs, core, kh, grp(g)]
        return pltpu.make_async_remote_copy(blk, blk, sd.at[l, zs, g, kh], rd.at[l, zs, g, kh],
                                            device_id={'dap': cpart}, device_id_type=MESH)

    def cp_z(l, up, h, g, kh, zs, dev):
        blk = b_ref.at[l, zs, c, kh, grp(g)]
        return pltpu.make_async_remote_copy(blk, blk, sz.at[l, int(up), h, g, kh], rz.at[l, int(up), h, g, kh],
                                            device_id={'dap': dev}, device_id_type=MESH)

    def send_z(l, up, h, g, kh):
        zs, zd = (z - h, z + 1) if up else (z + h, z - 1)
        return cp_z(l, up, h, g, kh, zs, dap_of(zd, y, c))

    def can_send(up, h):
        return (z - h >= 0) & (z + 1 < NZ) if up else (z + h < NZ) & (z - 1 >= 0)

    def can_recv(up, h):
        return z - h - 1 >= 0 if up else z + h + 1 < NZ

    def arrive(l, h, g, kh):
        for up in (False, True):
            @pl.when(can_recv(up, h))
            def _():
                zs = z - h - 1 if up else z + h + 1
                cp_z(l, up, h, g, kh, zs, cpart).wait_recv()
                cp_d(l, zs, g, kh, c).start()

    def forward(l, h, g):
        for up in (False, True):
            @pl.when(can_send(up, h + 1))
            def _():
                for kh in range(2):
                    send_z(l, up, h + 1, g, kh).start()

    def g_start(l):
        for r in range(1, NZ):
            g_z(l, r).start()
        g_own(l).start()

    g_start(0)
    g_fwd(0, 0, 0).start()
    g_fwd(0, 0, 1).start()
    g_start(1)

    r_i = lax.broadcasted_iota(jnp.int32, (256, 256), 0)
    c_i = lax.broadcasted_iota(jnp.int32, (256, 256), 1)
    perm = ((r_i // 16 == c_i % 16) & (r_i % 16 == c_i // 16)).astype(F32).astype(BF16)

    def turn(w):
        return w.astype(F32).T.astype(BF16)

    def prepare(l):
        rows = [bq_ref[l:l + 1, :], ni_ref[l, 0:1, :], ni_ref[l, 1:2, :], bo_ref[l:l + 1, :], bgate_ref[l:l + 1, :]]
        rows = rows + [bab_ref[l, qq:qq + 1, :] for qq in range(4)]
        rows = [v.astype(F32) for v in rows] + [jnp.zeros((7, 128), F32)]
        cols_ref[l] = jnp.concatenate(rows, axis=0).T
        for n in range(2):
            no_ref[l, n] = jnp.broadcast_to(nout_ref[l, n:n + 1, :].astype(F32), (128, 128)).T

        @pl.loop(0, 4)
        def _(blk):
            r2 = lax.broadcasted_iota(jnp.int32, (256, 1024), 0)
            k2 = lax.broadcasted_iota(jnp.int32, (256, 1024), 1)
            sel = ((k2 // 32 == r2 % 32) & (k2 % 32 == r2 // 32 + blk * 8)).astype(F32).astype(BF16)
            w = jnp.dot(sel, wq_ref[l], preferred_element_type=F32)
            wqt_ref[l, :, pl.ds(pl.multiple_of(blk * 256, 256), 256)] = w.T.astype(BF16)
        for qq in range(4):
            w = turn(wab_ref[l, :, qq * 128:(qq + 1) * 128])
            wabt_ref[l, :, qq * CC:(qq + 1) * CC, :] = w.reshape(NT, CC, 128)
        wgt_ref[l] = turn(wg_ref[l])
        wot_ref[l] = turn(wo_ref[l])

    def outer(l, kh):
        @pl.loop(0, 8, unroll=8)
        def _(dpp):
            half = pl.ds(kh * 128, 128)
            bt = jnp.concatenate([bg_ref[l, dpp * 2, half, :], bg_ref[l, dpp * 2 + 1, half, :]], axis=0)
            for par in range(2):
                for h in range(2):
                    rows = lax.dot_general(al_ref[l, pl.ds(par * 512 + h * 256, 256), :], bt, NTD,
                                           preferred_element_type=F32)
                    rows = (rows * (1.0 / 64)).astype(BF16).reshape(4, 2, 32, 256)
                    for e in range(2):
                        at = pl.ds(pl.multiple_of((dpp * 4 + e * 2 + par) * 32, 32), 32)
                        for i2 in range(2):
                            q_ref[pl.ds(h * 4, 4), at, i2 * 128:(i2 + 1) * 128] = rows[:, i2, :, e * 128:(e + 1) * 128]

        src = zt_ref if l == 0 else out_ref

        def rows(ip, _):
            upd = jnp.dot(wqt_ref[l], q_ref[ip], preferred_element_type=F32) + cols_ref[l, :, 0:1]
            zi = (src[kh, ip].astype(F32) + upd.astype(BF16).astype(F32)).astype(BF16)
            out_ref[kh, ip] = zi
            x = zi.astype(F32)
            xc = x - jnp.mean(x, axis=0, keepdims=True)
            var = jnp.mean(xc * xc, axis=0, keepdims=True)
            zn_ref[kh, ip] = (xc * lax.rsqrt(var + EPS) * cols_ref[l, :, 1:2] + cols_ref[l, :, 2:3]).astype(BF16)
            return 0

        lax.fori_loop(0, 8, rows, 0, unroll=8)

    def project(l, kh):
        def chunk(t, _):
            bias = jnp.concatenate([jnp.broadcast_to(cols_ref[l, sixteen(t), 5 + qq:6 + qq], (CC, 256))
                                    for qq in range(4)], axis=0)
            w = wabt_ref[l, t]

            def rows(ip, _):
                p = jnp.dot(w, zn_ref[kh, ip], preferred_element_type=F32) + bias
                m = mask_ref[kh, ip]
                at = (m * jax.nn.sigmoid(p[16:32]) * p[0:16]).astype(BF16)
                bt = (m * jax.nn.sigmoid(p[48:64]) * p[32:48]).astype(BF16)
                for i2 in range(2):
                    ln = slice(i2 * 128, (i2 + 1) * 128)
                    st_ref[sixteen(ip * 2 + i2), 0:128] = at[:, ln]
                    st_ref[sixteen(ip * 2 + i2), 128:256] = bt[:, ln]
                return 0

            lax.fori_loop(0, 8, rows, 0, unroll=8)
            ab = jnp.dot(perm, st_ref[...], preferred_element_type=F32).astype(BF16)
            aown_ref[l, kh, t] = ab[:, 0:128]
            b_ref[l, z, c, kh, t] = ab[:, 128:256]
            return 0

        @pl.loop(0, NG)
        def _(g):
            lax.fori_loop(g * TG, g * TG + TG, chunk, 0)
            for up in (False, True):
                @pl.when(can_send(up, 0))
                def _():
                    send_z(l, up, 0, g, kh).start()
            cp_a(l, g, kh).start()
            cp_d(l, z, g, kh, c).start()

    def ready(l, g):
        for kh in range(2):
            cp_a(l, g, kh).wait_recv()
            for zs in range(NZ):
                cp_d(l, zs, g, kh, 1 - c).wait_recv()

    def multiply(l, t):
        for cc in range(CC):
            rs = pl.ds(cc * 16, 16)
            lhs = jnp.concatenate([jnp.concatenate([r[l, kh, t, rs, :] for kh in range(2)], axis=1)
                                   for r in (aown_ref, arecv_ref)], axis=0)
            rhs = jnp.concatenate([jnp.concatenate([b_ref[l, zs, k, kh, t, rs, :] for kh in range(2)], axis=1)
                                   for zs in range(NZ) for k in range(2)], axis=0)
            o = lax.dot_general(lhs, rhs, NTD, preferred_element_type=F32)
            obuf_ref[l, y, t, rs, :] = o[0:16]
            osend_ref[l, t, rs, :] = o[16:32]
        cp_o(l, t).start()

    def drain(l):
        @pl.loop(0, NT)
        def _(t):
            cp_o(l, t).wait()

        @pl.loop(0, NG)
        def _(g):
            for kh in range(2):
                cp_a(l, g, kh).wait_send()
                for zs in range(NZ):
                    cp_d(l, zs, g, kh, c).wait_send()
                for up in (False, True):
                    for h in range(NZ - 1):
                        @pl.when(can_send(up, h))
                        def _():
                            send_z(l, up, h, g, kh).wait_send()

    def finish(l):
        def load(t, cc, hh):
            return obuf_ref[l, hh, t, pl.ds(cc * 16, 16), :]

        zero = jnp.zeros((16, 128), F32)

        def add1(t, s):
            for cc in range(CC):
                s = tuple(s[hh] + load(t, cc, hh) for hh in range(2))
            return s

        tot = lax.fori_loop(0, NT, add1, (zero, zero), unroll=2)
        mean = tuple(s * (1.0 / 128) for s in tot)

        def add2(t, s):
            for cc in range(CC):
                d = tuple(load(t, cc, hh) - mean[hh] for hh in range(2))
                s = tuple(s[hh] + d[hh] * d[hh] for hh in range(2))
            return s

        sq = lax.fori_loop(0, NT, add2, (zero, zero), unroll=2)
        inv = tuple(lax.rsqrt(s * (1.0 / 128) + EPS) for s in sq)

        def norm(t, _):
            for cc in range(CC):
                for hh in range(2):
                    one = pl.ds(t * CC + cc, 1)
                    v = (load(t, cc, hh) - mean[hh]) * inv[hh] * no_ref[l, 0, one, :] + no_ref[l, 1, one, :]
                    ost_ref[pl.ds(cc * 16, 16), pl.ds(hh * 128, 128)] = v.astype(BF16)
            on = jnp.dot(perm, ost_ref[...], preferred_element_type=F32).astype(BF16).reshape(8, 2, CC, 256)
            for hh in range(2):
                for i2 in range(2):
                    on_ref[hh, :, sixteen(t), i2 * 128:(i2 + 1) * 128] = on[:, i2, :, hh * 128:(hh + 1) * 128]
            return 0

        lax.fori_loop(0, NT, norm, 0, unroll=2)

        for kh in range(2):
            def rows(ip, _):
                u = (jnp.dot(wot_ref[l], on_ref[kh, ip], preferred_element_type=F32) + cols_ref[l, :, 3:4]).astype(BF16)
                g = jax.nn.sigmoid(jnp.dot(wgt_ref[l], zn_ref[kh, ip], preferred_element_type=F32)
                                   + cols_ref[l, :, 4:5])
                out_ref[kh, ip] = (out_ref[kh, ip].astype(F32) + g * u.astype(F32)).astype(BF16)
                return 0

            lax.fori_loop(0, 8, rows, 0, unroll=8)

    prepare(0)
    m = maskin_ref[...].astype(F32)
    for kh in range(2):
        half = jnp.concatenate([m[:, zz * 64 + kh * 32:zz * 64 + kh * 32 + 32] for zz in range(NZ)], axis=1)
        for i in range(16):
            mask_ref[kh, i // 2, :, i % 2 * 128:(i % 2 + 1) * 128] = half[i:i + 1, :]
    g_pass_z(0)
    g_pass_y(0)
    g_finish(0)
    for l in range(NL):
        for kh in range(2):
            outer(l, kh)
            project(l, kh)
        @pl.loop(0, NG)
        def _(g):
            arrive(l, 0, g, 0)

        @pl.loop(0, NG)
        def _(g):
            arrive(l, 0, g, 1)
            forward(l, 0, g)

        if l == 0:
            g_fwd(1, 0, 0).start()
            g_fwd(1, 0, 1).start()
            g_pass_z(1)
            prepare(1)

        @pl.loop(0, NG)
        def _(g):
            for kh in range(2):
                arrive(l, 1, g, kh)
            forward(l, 1, g)

        if l == 0:
            g_pass_y(1)
            g_finish(1)

        @pl.loop(0, NG)
        def _(g):
            for kh in range(2):
                arrive(l, 2, g, kh)
            ready(l, g)

            @pl.loop(0, TG)
            def _(k):
                multiply(l, g * TG + k)

        drain(l)
        finish(l)


def solution(mesh):
    pair_spec = P(('batch', 'dap'), None, None)
    mask_spec = P(('batch', 'dap'), None)
    msa_spec = P(None, ('batch', 'dap'), None)
    vm = pl.BlockSpec(memory_space=pltpu.VMEM)
    dma = pltpu.SemaphoreType.DMA

    def bf(*shape):
        return pltpu.VMEM(shape, BF16)

    def f3(*shape):
        return pltpu.VMEM(shape, F32)

    call = pl.pallas_call(
        kernel,
        out_shape=jax.ShapeDtypeStruct((2, 8, 128, 256), BF16),
        in_specs=[vm] * 14,
        out_specs=vm,
        scratch_shapes=[
            f3(NL, 128, 16), f3(NL, 2, 128, 128), f3(2, 8, 1, 256),
            bf(NL, 16, 256, 128), bf(8, 1024, 256),
            bf(NL, 128, 1024), bf(NL, NT, 4 * CC, 128), bf(NL, 128, 128), bf(NL, 128, 128),
            bf(2, 8, 128, 256), bf(256, 256),
            bf(NL, 2, NT, 256, 128), bf(NL, 2, NT, 256, 128), bf(NL, NZ, 2, 2, NT, 256, 128),
            f3(NL, 2, NT, 256, 128), f3(NL, NT, 256, 128), bf(256, 256), bf(2, 8, 128, 256),
            dma((NL, 8)), dma((NL, 8)), dma((NL, 8)), dma((NL, 8)), dma((NL,)),
            dma((NL, NG, 2)), dma((NL, NG, 2)),
            dma((NL, 2, NZ - 1, NG, 2)), dma((NL, 2, NZ - 1, NG, 2)),
            dma((NL, NZ, NG, 2)), dma((NL, NZ, NG, 2)),
            dma((NL, NT)), dma((NL, NT)),
        ],
        compiler_params=pltpu.CompilerParams(collective_id=0, has_side_effects=True),
        name='layers',
    )

    def device_fn(pair, mask, msa, opm_norm, opm_w_in, opm_b_in, opm_w_out, opm_b_out, tri_norm_in, tri_w_ab, tri_b_ab,
                  tri_w_gate, tri_b_gate, tri_norm_out, tri_w_out, tri_b_out):
        x = msa.astype(F32)
        xc = x - jnp.mean(x, axis=-1, keepdims=True)
        var = jnp.mean(xc * xc, axis=-1, keepdims=True)
        xh = xc * lax.rsqrt(var + EPS)
        nw = opm_norm.astype(F32)
        mn = (xh[None] * nw[:, 0][:, None, None] + nw[:, 1][:, None, None]).astype(BF16)
        bias = opm_b_in.astype(F32)
        b = (jnp.einsum('lmd,lsjm->ldjs', opm_w_in[:, :, 1], mn, preferred_element_type=F32)
             + bias[:, 1][:, :, None, None]).astype(BF16)
        b = b.reshape(2, 16, 2, 16, 64).transpose(0, 1, 3, 2, 4).reshape(2, 16, 16, 128)
        a = (jnp.einsum('lmc,lsim->lics', opm_w_in[:, :, 0], mn, preferred_element_type=F32)
             + bias[:, 0][:, None, :, None]).astype(BF16).reshape(2, 512, 64)
        al = jnp.concatenate([jnp.pad(a, ((0, 0), (0, 0), (0, 64))), jnp.pad(a, ((0, 0), (0, 0), (64, 0)))], axis=1)

        zt = pair.reshape(8, 2, 4, 2, 32, 128).transpose(3, 0, 5, 1, 2, 4).reshape(2, 8, 128, 256)
        zt = call(zt, mask, al, b, opm_w_out, tri_w_ab.reshape(2, 128, 512), tri_w_gate, tri_w_out,
                  opm_b_out, tri_norm_in, tri_b_out, tri_b_gate, tri_b_ab, tri_norm_out)
        return zt.reshape(2, 8, 128, 2, 4, 32).transpose(1, 3, 4, 0, 5, 2).reshape(16, 256, 128)

    return jax.shard_map(device_fn, mesh=mesh, in_specs=(pair_spec, mask_spec, msa_spec) + (P(),) * 13,
                         out_specs=pair_spec, check_vma=False)
```

```python
import jax
import jax.numpy as jnp
from jax import lax
from jax.sharding import PartitionSpec as P
from jax.experimental import pallas as pl
from jax.experimental.pallas import tpu as pltpu

EPS = 1e-5
MESH = pl.DeviceIdType.MESH
F32, BF16 = jnp.float32, jnp.bfloat16
NL = 2
NT = 8
CC = 16
TG = 1
NG = NT // TG
NZ = 4

NTD = (((1,), (1,)), ((), ()))


def place():
    me = lax.axis_index('dap')
    return me // 4, (me // 2) % 2, me % 2


def dap_of(z, y, c):
    return (z * 2 + y) * 2 + c


def sixteen(i):
    return pl.ds(pl.multiple_of(i * 16, 16), 16)


def kernel(zt_ref, maskin_ref, al_ref, bown_ref, wq_ref, wab_ref, wg_ref, wo_ref,
           bq_ref, ni_ref, bo_ref, bgate_ref, bab_ref, nout_ref,
           out_ref,
           cols_ref, no_ref, mask_ref, bg_ref, q_ref, wqt_ref, wabt_ref, wgt_ref, wot_ref, zn_ref, st_ref, aown_ref, arecv_ref, b_ref,
           obuf_ref, osend_ref, ost_ref, on_ref,
           sgi, rgi, sgd, rgd, sown, sa, ra, sz, rz, sd, rd, so, ro):
    z, y, c = place()
    ypart = dap_of(z, 1 - y, c)
    cpart = dap_of(z, y, 1 - c)

    bar = pltpu.get_barrier_semaphore()
    for r in range(1, NZ):
        pl.semaphore_signal(bar, inc=1, device_id={'dap': dap_of(lax.rem(z + r, NZ), y, c)}, device_id_type=MESH)
    pl.semaphore_signal(bar, inc=1, device_id={'dap': ypart}, device_id_type=MESH)
    pl.semaphore_signal(bar, inc=1, device_id={'dap': cpart}, device_id_type=MESH)
    pl.semaphore_wait(bar, NZ + 1)

    def bslot(l, zz, yy, core):
        return bg_ref.at[l, :, sixteen((yy * NZ + zz) * 2 + core), :]

    def g_z(l, r):
        return pltpu.make_async_remote_copy(
            bown_ref.at[l], bslot(l, z, y, c), sgi.at[l, r], rgi.at[l, r],
            device_id={'dap': dap_of(lax.rem(z + r, NZ), y, c)}, device_id_type=MESH)

    def g_fwd(l, r, other):
        zs = lax.rem(z - r + NZ, NZ)
        src = bown_ref.at[l] if r == 0 else bslot(l, zs, y, c)
        if other == 0:
            return pltpu.make_async_remote_copy(src, bslot(l, zs, y, c), sgi.at[l, NZ + r], rgi.at[l, NZ + r],
                                                device_id={'dap': ypart}, device_id_type=MESH)
        if other == 1:
            return pltpu.make_async_remote_copy(src, bslot(l, zs, y, c), sgd.at[l, r], rgd.at[l, r],
                                                device_id={'dap': cpart}, device_id_type=MESH)
        far = bslot(l, zs, 1 - y, c)
        return pltpu.make_async_remote_copy(far, far, sgd.at[l, NZ + r], rgd.at[l, NZ + r],
                                            device_id={'dap': cpart}, device_id_type=MESH)

    def g_own(l):
        return pltpu.make_async_copy(bown_ref.at[l], bslot(l, z, y, c), sown.at[l])

    def g_pass_z(l):
        for r in range(1, NZ):
            g_z(l, r).wait_recv()
            g_fwd(l, r, 0).start()
            g_fwd(l, r, 1).start()

    def g_pass_y(l):
        for r in range(NZ):
            g_fwd(l, r, 0).wait_recv()
            g_fwd(l, r, 2).start()

    def g_finish(l):
        g_own(l).wait()
        for r in range(NZ):
            g_fwd(l, r, 1).wait()
            g_fwd(l, r, 2).wait()
            g_fwd(l, r, 0).wait_send()
            if r > 0:
                g_z(l, r).wait_send()

    def grp(g):
        return pl.ds(g * TG, TG)

    def cp_a(l, g, kh):
        return pltpu.make_async_remote_copy(aown_ref.at[l, kh, grp(g)], arecv_ref.at[l, kh, grp(g)], sa.at[l, g, kh],
                                            ra.at[l, g, kh], device_id={'dap': ypart}, device_id_type=MESH)

    def cp_o(l, t):
        return pltpu.make_async_remote_copy(osend_ref.at[l, t], obuf_ref.at[l, y, t], so.at[l, t], ro.at[l, t],
                                            device_id={'dap': ypart}, device_id_type=MESH)

    def cp_d(l, zs, g, kh, core):
        blk = b_ref.at[l, zs, core, kh, grp(g)]
        return pltpu.make_async_remote_copy(blk, blk, sd.at[l, zs, g, kh], rd.at[l, zs, g, kh],
                                            device_id={'dap': cpart}, device_id_type=MESH)

    def cp_z(l, up, h, g, kh, zs, dev):
        blk = b_ref.at[l, zs, c, kh, grp(g)]
        return pltpu.make_async_remote_copy(blk, blk, sz.at[l, int(up), h, g, kh], rz.at[l, int(up), h, g, kh],
                                            device_id={'dap': dev}, device_id_type=MESH)

    def send_z(l, up, h, g, kh):
        zs, zd = (z - h, z + 1) if up else (z + h, z - 1)
        return cp_z(l, up, h, g, kh, zs, dap_of(zd, y, c))

    def can_send(up, h):
        return (z - h >= 0) & (z + 1 < NZ) if up else (z + h < NZ) & (z - 1 >= 0)

    def can_recv(up, h):
        return z - h - 1 >= 0 if up else z + h + 1 < NZ

    def on_side(up, side):
        return (z >= 2) if (up == (side == 0)) else (z < 2)

    def arrive(l, h, g, kh, side):
        for up in (False, True):
            @pl.when(can_recv(up, h) & on_side(up, side))
            def _():
                zs = z - h - 1 if up else z + h + 1
                cp_z(l, up, h, g, kh, zs, cpart).wait_recv()
                cp_d(l, zs, g, kh, c).start()

    def forward(l, h, g, side):
        for up in (False, True):
            @pl.when(can_send(up, h + 1) & on_side(up, side))
            def _():
                for kh in range(2):
                    send_z(l, up, h + 1, g, kh).start()

    def g_start(l):
        for r in range(1, NZ):
            g_z(l, r).start()
        g_own(l).start()

    g_start(0)
    g_fwd(0, 0, 0).start()
    g_fwd(0, 0, 1).start()
    g_start(1)

    r_i = lax.broadcasted_iota(jnp.int32, (256, 256), 0)
    c_i = lax.broadcasted_iota(jnp.int32, (256, 256), 1)
    perm = ((r_i // 16 == c_i % 16) & (r_i % 16 == c_i // 16)).astype(F32).astype(BF16)

    def turn(w):
        return w.astype(F32).T.astype(BF16)

    def prepare(l):
        rows = [bq_ref[l:l + 1, :], ni_ref[l, 0:1, :], ni_ref[l, 1:2, :], bo_ref[l:l + 1, :], bgate_ref[l:l + 1, :]]
        rows = rows + [bab_ref[l, qq:qq + 1, :] for qq in range(4)]
        rows = [v.astype(F32) for v in rows] + [jnp.zeros((7, 128), F32)]
        cols_ref[l] = jnp.concatenate(rows, axis=0).T
        for n in range(2):
            no_ref[l, n] = jnp.broadcast_to(nout_ref[l, n:n + 1, :].astype(F32), (128, 128)).T

        @pl.loop(0, 4)
        def _(blk):
            r2 = lax.broadcasted_iota(jnp.int32, (256, 1024), 0)
            k2 = lax.broadcasted_iota(jnp.int32, (256, 1024), 1)
            sel = ((k2 // 32 == r2 % 32) & (k2 % 32 == r2 // 32 + blk * 8)).astype(F32).astype(BF16)
            w = jnp.dot(sel, wq_ref[l], preferred_element_type=F32)
            wqt_ref[l, :, pl.ds(pl.multiple_of(blk * 256, 256), 256)] = w.T.astype(BF16)
        for qq in range(4):
            w = turn(wab_ref[l, :, qq * 128:(qq + 1) * 128])
            wabt_ref[l, :, qq * CC:(qq + 1) * CC, :] = w.reshape(NT, CC, 128)
        wgt_ref[l] = turn(wg_ref[l])
        wot_ref[l] = turn(wo_ref[l])

    def outer(l, kh):
        @pl.loop(0, 8, unroll=8)
        def _(dpp):
            half = pl.ds(kh * 128, 128)
            bt = jnp.concatenate([bg_ref[l, dpp * 2, half, :], bg_ref[l, dpp * 2 + 1, half, :]], axis=0)
            for par in range(2):
                for h in range(2):
                    rows = lax.dot_general(al_ref[l, pl.ds(par * 512 + h * 256, 256), :], bt, NTD,
                                           preferred_element_type=F32)
                    rows = (rows * (1.0 / 64)).astype(BF16).reshape(4, 2, 32, 256)
                    for e in range(2):
                        at = pl.ds(pl.multiple_of((dpp * 4 + e * 2 + par) * 32, 32), 32)
                        for i2 in range(2):
                            q_ref[pl.ds(h * 4, 4), at, i2 * 128:(i2 + 1) * 128] = rows[:, i2, :, e * 128:(e + 1) * 128]

        src = zt_ref if l == 0 else out_ref

        def rows(ip, _):
            upd = jnp.dot(wqt_ref[l], q_ref[ip], preferred_element_type=F32) + cols_ref[l, :, 0:1]
            zi = (src[kh, ip].astype(F32) + upd.astype(BF16).astype(F32)).astype(BF16)
            out_ref[kh, ip] = zi
            x = zi.astype(F32)
            xc = x - jnp.mean(x, axis=0, keepdims=True)
            var = jnp.mean(xc * xc, axis=0, keepdims=True)
            zn_ref[kh, ip] = (xc * lax.rsqrt(var + EPS) * cols_ref[l, :, 1:2] + cols_ref[l, :, 2:3]).astype(BF16)
            return 0

        lax.fori_loop(0, 8, rows, 0, unroll=8)

    def project(l, kh):
        def chunk(t, _):
            bias = jnp.concatenate([jnp.broadcast_to(cols_ref[l, sixteen(t), 5 + qq:6 + qq], (CC, 256))
                                    for qq in range(4)], axis=0)
            w = wabt_ref[l, t]

            def rows(ip, _):
                p = jnp.dot(w, zn_ref[kh, ip], preferred_element_type=F32) + bias
                m = mask_ref[kh, ip]
                at = (m * jax.nn.sigmoid(p[16:32]) * p[0:16]).astype(BF16)
                bt = (m * jax.nn.sigmoid(p[48:64]) * p[32:48]).astype(BF16)
                for i2 in range(2):
                    ln = slice(i2 * 128, (i2 + 1) * 128)
                    st_ref[sixteen(ip * 2 + i2), 0:128] = at[:, ln]
                    st_ref[sixteen(ip * 2 + i2), 128:256] = bt[:, ln]
                return 0

            lax.fori_loop(0, 8, rows, 0, unroll=8)
            ab = jnp.dot(perm, st_ref[...], preferred_element_type=F32).astype(BF16)
            aown_ref[l, kh, t] = ab[:, 0:128]
            b_ref[l, z, c, kh, t] = ab[:, 128:256]
            return 0

        @pl.loop(0, NG)
        def _(g):
            lax.fori_loop(g * TG, g * TG + TG, chunk, 0)
            for up in (False, True):
                @pl.when(can_send(up, 0))
                def _():
                    send_z(l, up, 0, g, kh).start()
            cp_a(l, g, kh).start()
            cp_d(l, z, g, kh, c).start()

    def ready(l, g):
        for kh in range(2):
            cp_a(l, g, kh).wait_recv()
            for zs in range(NZ):
                cp_d(l, zs, g, kh, 1 - c).wait_recv()

    def multiply(l, t):
        for cc in range(CC):
            rs = pl.ds(cc * 16, 16)
            lhs = jnp.concatenate([jnp.concatenate([r[l, kh, t, rs, :] for kh in range(2)], axis=1)
                                   for r in (aown_ref, arecv_ref)], axis=0)
            rhs = jnp.concatenate([jnp.concatenate([b_ref[l, zs, k, kh, t, rs, :] for kh in range(2)], axis=1)
                                   for zs in range(NZ) for k in range(2)], axis=0)
            o = lax.dot_general(lhs, rhs, NTD, preferred_element_type=F32)
            obuf_ref[l, y, t, rs, :] = o[0:16]
            osend_ref[l, t, rs, :] = o[16:32]
        cp_o(l, t).start()

    def drain(l):
        @pl.loop(0, NT)
        def _(t):
            cp_o(l, t).wait_send()

        @pl.loop(0, NG)
        def _(g):
            for kh in range(2):
                cp_a(l, g, kh).wait_send()
                for zs in range(NZ):
                    cp_d(l, zs, g, kh, c).wait_send()
                for up in (False, True):
                    for h in range(NZ - 1):
                        @pl.when(can_send(up, h))
                        def _():
                            send_z(l, up, h, g, kh).wait_send()

    def finish(l):
        def load(t, cc, hh):
            return obuf_ref[l, hh, t, pl.ds(cc * 16, 16), :]

        zero = jnp.zeros((16, 128), F32)

        def add1(t, s):
            for cc in range(CC):
                s = tuple(s[hh] + load(t, cc, hh) for hh in range(2))
            return s

        tot = lax.fori_loop(0, NT, add1, (zero, zero), unroll=2)
        mean = tuple(s * (1.0 / 128) for s in tot)

        def add2(t, s):
            for cc in range(CC):
                d = tuple(load(t, cc, hh) - mean[hh] for hh in range(2))
                s = tuple(s[hh] + d[hh] * d[hh] for hh in range(2))
            return s

        sq = lax.fori_loop(0, NT, add2, (zero, zero), unroll=2)
        inv = tuple(lax.rsqrt(s * (1.0 / 128) + EPS) for s in sq)

        def norm(t, _):
            for cc in range(CC):
                for hh in range(2):
                    one = pl.ds(t * CC + cc, 1)
                    v = (load(t, cc, hh) - mean[hh]) * inv[hh] * no_ref[l, 0, one, :] + no_ref[l, 1, one, :]
                    ost_ref[pl.ds(cc * 16, 16), pl.ds(hh * 128, 128)] = v.astype(BF16)
            on = jnp.dot(perm, ost_ref[...], preferred_element_type=F32).astype(BF16).reshape(8, 2, CC, 256)
            for hh in range(2):
                for i2 in range(2):
                    on_ref[hh, :, sixteen(t), i2 * 128:(i2 + 1) * 128] = on[:, i2, :, hh * 128:(hh + 1) * 128]
            return 0

        lax.fori_loop(0, NT, norm, 0, unroll=2)

        for kh in range(2):
            def rows(ip, _):
                u = (jnp.dot(wot_ref[l], on_ref[kh, ip], preferred_element_type=F32) + cols_ref[l, :, 3:4]).astype(BF16)
                g = jax.nn.sigmoid(jnp.dot(wgt_ref[l], zn_ref[kh, ip], preferred_element_type=F32)
                                   + cols_ref[l, :, 4:5])
                out_ref[kh, ip] = (out_ref[kh, ip].astype(F32) + g * u.astype(F32)).astype(BF16)
                return 0

            lax.fori_loop(0, 8, rows, 0, unroll=8)

    prepare(0)
    m = maskin_ref[...].astype(F32)
    for kh in range(2):
        half = jnp.concatenate([m[:, zz * 64 + kh * 32:zz * 64 + kh * 32 + 32] for zz in range(NZ)], axis=1)
        for i in range(16):
            mask_ref[kh, i // 2, :, i % 2 * 128:(i % 2 + 1) * 128] = half[i:i + 1, :]
    g_pass_z(0)
    g_pass_y(0)
    g_finish(0)
    for l in range(NL):
        for kh in range(2):
            outer(l, kh)
            project(l, kh)
        for side in range(2):
            @pl.loop(0, NG)
            def _(g):
                arrive(l, 0, g, 0, side)

            @pl.loop(0, NG)
            def _(g):
                arrive(l, 0, g, 1, side)
                forward(l, 0, g, side)

            if l == 0 and side == 0:
                g_fwd(1, 0, 0).start()
                g_fwd(1, 0, 1).start()
                g_pass_z(1)
                prepare(1)

        @pl.loop(0, NG)
        def _(g):
            for kh in range(2):
                arrive(l, 1, g, kh, 0)
            forward(l, 1, g, 0)

        if l == 0:
            g_pass_y(1)
            g_finish(1)

        @pl.loop(0, NG)
        def _(g):
            for kh in range(2):
                arrive(l, 2, g, kh, 0)
            ready(l, g)

            @pl.loop(0, TG)
            def _(k):
                multiply(l, g * TG + k)

        @pl.loop(0, NT)
        def _(t):
            cp_o(l, t).wait_recv()

        finish(l)

    for l in range(NL):
        drain(l)


def solution(mesh):
    pair_spec = P(('batch', 'dap'), None, None)
    mask_spec = P(('batch', 'dap'), None)
    msa_spec = P(None, ('batch', 'dap'), None)
    vm = pl.BlockSpec(memory_space=pltpu.VMEM)
    dma = pltpu.SemaphoreType.DMA

    def bf(*shape):
        return pltpu.VMEM(shape, BF16)

    def f3(*shape):
        return pltpu.VMEM(shape, F32)

    call = pl.pallas_call(
        kernel,
        out_shape=jax.ShapeDtypeStruct((2, 8, 128, 256), BF16),
        in_specs=[vm] * 14,
        out_specs=vm,
        scratch_shapes=[
            f3(NL, 128, 16), f3(NL, 2, 128, 128), f3(2, 8, 1, 256),
            bf(NL, 16, 256, 128), bf(8, 1024, 256),
            bf(NL, 128, 1024), bf(NL, NT, 4 * CC, 128), bf(NL, 128, 128), bf(NL, 128, 128),
            bf(2, 8, 128, 256), bf(256, 256),
            bf(NL, 2, NT, 256, 128), bf(NL, 2, NT, 256, 128), bf(NL, NZ, 2, 2, NT, 256, 128),
            f3(NL, 2, NT, 256, 128), f3(NL, NT, 256, 128), bf(256, 256), bf(2, 8, 128, 256),
            dma((NL, 8)), dma((NL, 8)), dma((NL, 8)), dma((NL, 8)), dma((NL,)),
            dma((NL, NG, 2)), dma((NL, NG, 2)),
            dma((NL, 2, NZ - 1, NG, 2)), dma((NL, 2, NZ - 1, NG, 2)),
            dma((NL, NZ, NG, 2)), dma((NL, NZ, NG, 2)),
            dma((NL, NT)), dma((NL, NT)),
        ],
        compiler_params=pltpu.CompilerParams(collective_id=0, has_side_effects=True),
        name='layers',
    )

    def device_fn(pair, mask, msa, opm_norm, opm_w_in, opm_b_in, opm_w_out, opm_b_out, tri_norm_in, tri_w_ab, tri_b_ab,
                  tri_w_gate, tri_b_gate, tri_norm_out, tri_w_out, tri_b_out):
        x = msa.astype(F32)
        xc = x - jnp.mean(x, axis=-1, keepdims=True)
        var = jnp.mean(xc * xc, axis=-1, keepdims=True)
        xh = xc * lax.rsqrt(var + EPS)
        nw = opm_norm.astype(F32)
        mn = (xh[None] * nw[:, 0][:, None, None] + nw[:, 1][:, None, None]).astype(BF16)
        bias = opm_b_in.astype(F32)
        b = (jnp.einsum('lmd,lsjm->ldjs', opm_w_in[:, :, 1], mn, preferred_element_type=F32)
             + bias[:, 1][:, :, None, None]).astype(BF16)
        b = b.reshape(2, 16, 2, 16, 64).transpose(0, 1, 3, 2, 4).reshape(2, 16, 16, 128)
        a = (jnp.einsum('lmc,lsim->lics', opm_w_in[:, :, 0], mn, preferred_element_type=F32)
             + bias[:, 0][:, None, :, None]).astype(BF16).reshape(2, 512, 64)
        al = jnp.concatenate([jnp.pad(a, ((0, 0), (0, 0), (0, 64))), jnp.pad(a, ((0, 0), (0, 0), (64, 0)))], axis=1)

        zt = pair.reshape(8, 2, 4, 2, 32, 128).transpose(3, 0, 5, 1, 2, 4).reshape(2, 8, 128, 256)
        zt = call(zt, mask, al, b, opm_w_out, tri_w_ab.reshape(2, 128, 512), tri_w_gate, tri_w_out,
                  opm_b_out, tri_norm_in, tri_b_out, tri_b_gate, tri_b_ab, tri_norm_out)
        return zt.reshape(2, 8, 128, 2, 4, 32).transpose(1, 3, 4, 0, 5, 2).reshape(16, 256, 128)

    return jax.shard_map(device_fn, mesh=mesh, in_specs=(pair_spec, mask_spec, msa_spec) + (P(),) * 13,
                         out_specs=pair_spec, check_vma=False)
```

```python
import jax
import jax.numpy as jnp
from jax import lax
from jax.sharding import PartitionSpec as P
from jax.experimental import pallas as pl
from jax.experimental.pallas import tpu as pltpu

EPS = 1e-5
MESH = pl.DeviceIdType.MESH
F32, BF16 = jnp.float32, jnp.bfloat16
NL = 2
W = 128
W2 = 2 * W
NT = 8
CC = 16
TG = 1
NG = NT // TG
NZ = 4

NTD = (((1,), (1,)), ((), ()))


def place():
    me = lax.axis_index('dap')
    return me // 4, (me // 2) % 2, me % 2


def dap_of(z, y, c):
    return (z * 2 + y) * 2 + c


def sixteen(i):
    return pl.ds(pl.multiple_of(i * 16, 16), 16)


def kernel(pair_ref, maskin_ref, msa_ref, win_ref, onorm_ref, obin_ref, wq_ref, wab_ref, wg_ref, wo_ref,
           bq_ref, ni_ref, bo_ref, bgate_ref, bab_ref, nout_ref,
           out_ref,
           z_ref, al_ref, bown_ref, bst_ref, wt_ref, cols_ref, no_ref, mask_ref, bg_ref, q_ref, wqt_ref, wabt_ref, wgt_ref, wot_ref, zn_ref, st_ref, aown_ref, arecv_ref, b_ref,
           obuf_ref, osend_ref, ost_ref, on_ref,
           sgi, rgi, sgd, rgd, sown, sa, ra, sz, rz, sd, rd, so, ro):
    z, y, c = place()
    ypart = dap_of(z, 1 - y, c)
    cpart = dap_of(z, y, 1 - c)

    bar = pltpu.get_barrier_semaphore()
    for r in range(1, NZ):
        pl.semaphore_signal(bar, inc=1, device_id={'dap': dap_of(lax.rem(z + r, NZ), y, c)}, device_id_type=MESH)
    pl.semaphore_signal(bar, inc=1, device_id={'dap': ypart}, device_id_type=MESH)
    pl.semaphore_signal(bar, inc=1, device_id={'dap': cpart}, device_id_type=MESH)

    def turn(w):
        return w.astype(F32).T.astype(BF16)

    low = lax.broadcasted_iota(jnp.int32, (32, W), 1) < 64
    nul = jnp.zeros((32, W), F32)
    bcol = []
    for l in range(NL):
        wt_ref[l] = turn(win_ref[l])
        row = jnp.concatenate([obin_ref[l, 0:1, :].astype(F32), obin_ref[l, 1:2, :].astype(F32),
                               jnp.zeros((1, 64), F32)], axis=1)
        bcol.append(jnp.broadcast_to(row, (W, W)).T[0:64])

    def msa_row(i, _):
        x = msa_ref[i].astype(F32)
        xc = x - jnp.mean(x, axis=1, keepdims=True)
        var = jnp.mean(xc * xc, axis=1, keepdims=True)
        xh = xc * lax.rsqrt(var + EPS)
        for l in range(NL):
            mn = (xh * onorm_ref[l, 0:1, :].astype(F32) + onorm_ref[l, 1:2, :].astype(F32)).astype(BF16)
            ab = lax.dot_general(wt_ref[l], jnp.concatenate([mn, mn], axis=0), NTD, preferred_element_type=F32) + bcol[l]
            a = ab[0:32]
            al_ref[l, pl.ds(pl.multiple_of(i * 32, 32), 32), :] = jnp.where(low, a, nul).astype(BF16)
            al_ref[l, pl.ds(pl.multiple_of(512 + i * 32, 32), 32), :] = jnp.where(low, nul, a).astype(BF16)
            bst_ref[l, pl.ds(pl.multiple_of(i * 32, 32), 32), :] = ab[32:64].astype(BF16)
        return 0

    lax.fori_loop(0, 16, msa_row, 0, unroll=4)
    r_b = lax.broadcasted_iota(jnp.int32, (W2, 512), 0)
    k_b = lax.broadcasted_iota(jnp.int32, (W2, 512), 1)
    low_b = lax.broadcasted_iota(jnp.int32, (W2, W), 1) < 64
    sel_b = [((k_b // 32 == r_b % 16) & (k_b % 32 == r_b // 16 * 2 + par)).astype(F32).astype(BF16) for par in range(2)]
    for l in range(NL):
        v = [jnp.dot(sel_b[par], bst_ref[l], preferred_element_type=F32) for par in range(2)]
        bown_ref[l] = jnp.where(low_b, v[0], v[1]).astype(BF16).reshape(16, 16, W)

    pl.semaphore_wait(bar, NZ + 1)

    def bslot(l, zz, yy, core):
        return bg_ref.at[l, :, sixteen((yy * NZ + zz) * 2 + core), :]

    def g_z(l, r):
        return pltpu.make_async_remote_copy(
            bown_ref.at[l], bslot(l, z, y, c), sgi.at[l, r], rgi.at[l, r],
            device_id={'dap': dap_of(lax.rem(z + r, NZ), y, c)}, device_id_type=MESH)

    def g_fwd(l, r, other):
        zs = lax.rem(z - r + NZ, NZ)
        src = bown_ref.at[l] if r == 0 else bslot(l, zs, y, c)
        if other == 0:
            return pltpu.make_async_remote_copy(src, bslot(l, zs, y, c), sgi.at[l, NZ + r], rgi.at[l, NZ + r],
                                                device_id={'dap': ypart}, device_id_type=MESH)
        if other == 1:
            return pltpu.make_async_remote_copy(src, bslot(l, zs, y, c), sgd.at[l, r], rgd.at[l, r],
                                                device_id={'dap': cpart}, device_id_type=MESH)
        far = bslot(l, zs, 1 - y, c)
        return pltpu.make_async_remote_copy(far, far, sgd.at[l, NZ + r], rgd.at[l, NZ + r],
                                            device_id={'dap': cpart}, device_id_type=MESH)

    def g_own(l):
        return pltpu.make_async_copy(bown_ref.at[l], bslot(l, z, y, c), sown.at[l])

    def g_pass_z(l):
        for r in range(1, NZ):
            g_z(l, r).wait_recv()
            g_fwd(l, r, 0).start()
            g_fwd(l, r, 1).start()

    def g_pass_y(l):
        for r in range(NZ):
            g_fwd(l, r, 0).wait_recv()
            g_fwd(l, r, 2).start()

    def g_finish(l):
        g_own(l).wait()
        for r in range(NZ):
            g_fwd(l, r, 1).wait()
            g_fwd(l, r, 2).wait()
            g_fwd(l, r, 0).wait_send()
            if r > 0:
                g_z(l, r).wait_send()

    def grp(g):
        return pl.ds(g * TG, TG)

    def cp_a(l, g, kh):
        return pltpu.make_async_remote_copy(aown_ref.at[l, kh, grp(g)], arecv_ref.at[l, kh, grp(g)], sa.at[l, g, kh],
                                            ra.at[l, g, kh], device_id={'dap': ypart}, device_id_type=MESH)

    def cp_o(l, t):
        return pltpu.make_async_remote_copy(osend_ref.at[l, t], obuf_ref.at[l, y, t], so.at[l, t], ro.at[l, t],
                                            device_id={'dap': ypart}, device_id_type=MESH)

    def cp_d(l, zs, g, kh, core):
        blk = b_ref.at[l, zs, core, kh, grp(g)]
        return pltpu.make_async_remote_copy(blk, blk, sd.at[l, zs, g, kh], rd.at[l, zs, g, kh],
                                            device_id={'dap': cpart}, device_id_type=MESH)

    def cp_z(l, up, h, g, kh, zs, dev):
        blk = b_ref.at[l, zs, c, kh, grp(g)]
        return pltpu.make_async_remote_copy(blk, blk, sz.at[l, int(up), h, g, kh], rz.at[l, int(up), h, g, kh],
                                            device_id={'dap': dev}, device_id_type=MESH)

    def send_z(l, up, h, g, kh):
        zs, zd = (z - h, z + 1) if up else (z + h, z - 1)
        return cp_z(l, up, h, g, kh, zs, dap_of(zd, y, c))

    def can_send(up, h):
        return (z - h >= 0) & (z + 1 < NZ) if up else (z + h < NZ) & (z - 1 >= 0)

    def can_recv(up, h):
        return z - h - 1 >= 0 if up else z + h + 1 < NZ

    def arrive(l, h, g, kh):
        for up in (False, True):
            @pl.when(can_recv(up, h))
            def _():
                zs = z - h - 1 if up else z + h + 1
                cp_z(l, up, h, g, kh, zs, cpart).wait_recv()
                cp_d(l, zs, g, kh, c).start()

    def forward(l, h, g):
        for up in (False, True):
            @pl.when(can_send(up, h + 1))
            def _():
                for kh in range(2):
                    send_z(l, up, h + 1, g, kh).start()

    def g_start(l):
        for r in range(1, NZ):
            g_z(l, r).start()
        g_own(l).start()

    g_start(0)
    g_fwd(0, 0, 0).start()
    g_fwd(0, 0, 1).start()
    g_start(1)

    r_i = lax.broadcasted_iota(jnp.int32, (W2, W2), 0)
    c_i = lax.broadcasted_iota(jnp.int32, (W2, W2), 1)
    perm = ((r_i // 16 == c_i % 16) & (r_i % 16 == c_i // 16)).astype(F32).astype(BF16)

    def prepare(l):
        rows = [bq_ref[l:l + 1, :], ni_ref[l, 0:1, :], ni_ref[l, 1:2, :], bo_ref[l:l + 1, :], bgate_ref[l:l + 1, :]]
        rows = rows + [bab_ref[l, qq:qq + 1, :] for qq in range(4)]
        rows = [v.astype(F32) for v in rows] + [jnp.zeros((7, W), F32)]
        cols_ref[l] = jnp.concatenate(rows, axis=0).T
        for n in range(2):
            no_ref[l, n] = jnp.broadcast_to(nout_ref[l, n:n + 1, :].astype(F32), (W, W)).T

        @pl.loop(0, 4)
        def _(blk):
            r2 = lax.broadcasted_iota(jnp.int32, (W2, 1024), 0)
            k2 = lax.broadcasted_iota(jnp.int32, (W2, 1024), 1)
            sel = ((k2 // 32 == r2 % 32) & (k2 % 32 == r2 // 32 + blk * 8)).astype(F32).astype(BF16)
            w = jnp.dot(sel, wq_ref[l], preferred_element_type=F32)
            wqt_ref[l, :, pl.ds(pl.multiple_of(blk * W2, W2), W2)] = w.T.astype(BF16)
        for qq in range(4):
            w = turn(wab_ref[l, :, qq * W:(qq + 1) * W])
            wabt_ref[l, :, qq * CC:(qq + 1) * CC, :] = w.reshape(NT, CC, W)
        wgt_ref[l] = turn(wg_ref[l])
        wot_ref[l] = turn(wo_ref[l])

    def outer(l, kh):
        @pl.loop(0, 8, unroll=8)
        def _(dpp):
            half = pl.ds(kh * W, W)
            bt = jnp.concatenate([bg_ref[l, dpp * 2, half, :], bg_ref[l, dpp * 2 + 1, half, :]], axis=0)
            for par in range(2):
                for h in range(2):
                    rows = lax.dot_general(al_ref[l, pl.ds(par * 512 + h * W2, W2), :], bt, NTD,
                                           preferred_element_type=F32)
                    rows = (rows * (1.0 / 64)).astype(BF16).reshape(4, 2, 32, W2)
                    for e in range(2):
                        at = pl.ds(pl.multiple_of((dpp * 4 + e * 2 + par) * 32, 32), 32)
                        for i2 in range(2):
                            q_ref[pl.ds(h * 4, 4), at, i2 * W:(i2 + 1) * W] = rows[:, i2, :, e * W:(e + 1) * W]

        def rows(ip, _):
            upd = jnp.dot(wqt_ref[l], q_ref[ip], preferred_element_type=F32) + cols_ref[l, :, 0:1]
            zi = (z_ref[kh, ip].astype(F32) + upd.astype(BF16).astype(F32)).astype(BF16)
            z_ref[kh, ip] = zi
            x = zi.astype(F32)
            xc = x - jnp.mean(x, axis=0, keepdims=True)
            var = jnp.mean(xc * xc, axis=0, keepdims=True)
            zn_ref[kh, ip] = (xc * lax.rsqrt(var + EPS) * cols_ref[l, :, 1:2] + cols_ref[l, :, 2:3]).astype(BF16)
            return 0

        lax.fori_loop(0, 8, rows, 0, unroll=8)

    def project(l, kh):
        def chunk(t, _):
            bias = jnp.concatenate([jnp.broadcast_to(cols_ref[l, sixteen(t), 5 + qq:6 + qq], (CC, W2))
                                    for qq in range(4)], axis=0)
            w = wabt_ref[l, t]

            def rows(ip, _):
                p = jnp.dot(w, zn_ref[kh, ip], preferred_element_type=F32) + bias
                m = mask_ref[kh, ip]
                at = (m * jax.nn.sigmoid(p[16:32]) * p[0:16]).astype(BF16)
                bt = (m * jax.nn.sigmoid(p[48:64]) * p[32:48]).astype(BF16)
                for i2 in range(2):
                    ln = slice(i2 * W, (i2 + 1) * W)
                    st_ref[sixteen(ip * 2 + i2), 0:W] = at[:, ln]
                    st_ref[sixteen(ip * 2 + i2), W:W2] = bt[:, ln]
                return 0

            lax.fori_loop(0, 8, rows, 0, unroll=8)
            ab = jnp.dot(perm, st_ref[...], preferred_element_type=F32).astype(BF16)
            aown_ref[l, kh, t] = ab[:, 0:W]
            b_ref[l, z, c, kh, t] = ab[:, W:W2]
            return 0

        @pl.loop(0, NG)
        def _(g):
            lax.fori_loop(g * TG, g * TG + TG, chunk, 0)
            for up in (False, True):
                @pl.when(can_send(up, 0))
                def _():
                    send_z(l, up, 0, g, kh).start()
            cp_a(l, g, kh).start()
            cp_d(l, z, g, kh, c).start()

    def ready(l, g):
        for kh in range(2):
            cp_a(l, g, kh).wait_recv()
            for zs in range(NZ):
                cp_d(l, zs, g, kh, 1 - c).wait_recv()

    def multiply(l, t):
        for cc in range(CC):
            rs = pl.ds(cc * 16, 16)
            lhs = jnp.concatenate([jnp.concatenate([r[l, kh, t, rs, :] for kh in range(2)], axis=1)
                                   for r in (aown_ref, arecv_ref)], axis=0)
            rhs = jnp.concatenate([jnp.concatenate([b_ref[l, zs, k, kh, t, rs, :] for kh in range(2)], axis=1)
                                   for zs in range(NZ) for k in range(2)], axis=0)
            o = lax.dot_general(lhs, rhs, NTD, preferred_element_type=F32)
            obuf_ref[l, y, t, rs, :] = o[0:16]
            osend_ref[l, t, rs, :] = o[16:32]
        cp_o(l, t).start()

    def drain(l):
        @pl.loop(0, NT)
        def _(t):
            cp_o(l, t).wait()

        @pl.loop(0, NG)
        def _(g):
            for kh in range(2):
                cp_a(l, g, kh).wait_send()
                for zs in range(NZ):
                    cp_d(l, zs, g, kh, c).wait_send()
                for up in (False, True):
                    for h in range(NZ - 1):
                        @pl.when(can_send(up, h))
                        def _():
                            send_z(l, up, h, g, kh).wait_send()

    def finish(l):
        def load(t, cc, hh):
            return obuf_ref[l, hh, t, pl.ds(cc * 16, 16), :]

        zero = jnp.zeros((16, W), F32)

        def add1(t, s):
            for cc in range(CC):
                s = tuple(s[hh] + load(t, cc, hh) for hh in range(2))
            return s

        tot = lax.fori_loop(0, NT, add1, (zero, zero), unroll=2)
        mean = tuple(s * (1.0 / W) for s in tot)

        def add2(t, s):
            for cc in range(CC):
                d = tuple(load(t, cc, hh) - mean[hh] for hh in range(2))
                s = tuple(s[hh] + d[hh] * d[hh] for hh in range(2))
            return s

        sq = lax.fori_loop(0, NT, add2, (zero, zero), unroll=2)
        inv = tuple(lax.rsqrt(s * (1.0 / W) + EPS) for s in sq)

        def norm(t, _):
            for cc in range(CC):
                for hh in range(2):
                    one = pl.ds(t * CC + cc, 1)
                    v = (load(t, cc, hh) - mean[hh]) * inv[hh] * no_ref[l, 0, one, :] + no_ref[l, 1, one, :]
                    ost_ref[pl.ds(cc * 16, 16), pl.ds(hh * W, W)] = v.astype(BF16)
            on = jnp.dot(perm, ost_ref[...], preferred_element_type=F32).astype(BF16).reshape(8, 2, CC, W2)
            for hh in range(2):
                for i2 in range(2):
                    on_ref[hh, :, sixteen(t), i2 * W:(i2 + 1) * W] = on[:, i2, :, hh * W:(hh + 1) * W]
            return 0

        lax.fori_loop(0, NT, norm, 0, unroll=2)

        for kh in range(2):
            def rows(ip, _):
                u = (jnp.dot(wot_ref[l], on_ref[kh, ip], preferred_element_type=F32) + cols_ref[l, :, 3:4]).astype(BF16)
                g = jax.nn.sigmoid(jnp.dot(wgt_ref[l], zn_ref[kh, ip], preferred_element_type=F32)
                                   + cols_ref[l, :, 4:5])
                zi = z_ref[kh, ip].astype(F32) + g * u.astype(F32)
                if l < NL - 1:
                    z_ref[kh, ip] = zi.astype(BF16)
                else:
                    zo = zi.T.astype(BF16)
                    for i2 in range(2):
                        for zz in range(NZ):
                            out_ref[ip * 2 + i2, pl.ds(zz * 64 + kh * 32, 32), :] = zo[i2 * W + zz * 32:i2 * W + zz * 32 + 32]
                return 0

            lax.fori_loop(0, 8, rows, 0, unroll=8)

    prepare(0)
    m = maskin_ref[...].astype(F32)
    for kh in range(2):
        half = jnp.concatenate([m[:, zz * 64 + kh * 32:zz * 64 + kh * 32 + 32] for zz in range(NZ)], axis=1)
        for i in range(16):
            mask_ref[kh, i // 2, :, i % 2 * W:(i % 2 + 1) * W] = half[i:i + 1, :]

    def bring(ip, _):
        for kh in range(2):
            for i2 in range(2):
                rows = jnp.concatenate([pair_ref[ip * 2 + i2, pl.ds(zz * 64 + kh * 32, 32), :] for zz in range(NZ)], axis=0)
                z_ref[kh, ip, :, i2 * W:(i2 + 1) * W] = turn(rows)
        return 0

    g_pass_z(0)
    lax.fori_loop(0, 8, bring, 0, unroll=2)
    g_pass_y(0)
    g_finish(0)
    for l in range(NL):
        for kh in range(2):
            outer(l, kh)
            project(l, kh)
            if l == 0 and kh == 0:
                g_fwd(1, 0, 0).start()
                g_fwd(1, 0, 1).start()
                g_pass_z(1)
        if l == 0:
            prepare(1)
        @pl.loop(0, NG)
        def _(g):
            arrive(l, 0, g, 0)

        @pl.loop(0, NG)
        def _(g):
            arrive(l, 0, g, 1)
            forward(l, 0, g)

        @pl.loop(0, NG)
        def _(g):
            for kh in range(2):
                arrive(l, 1, g, kh)
            forward(l, 1, g)

        if l == 0:
            g_pass_y(1)

        @pl.loop(0, NG)
        def _(g):
            for kh in range(2):
                arrive(l, 2, g, kh)
            ready(l, g)

            @pl.loop(0, TG)
            def _(k):
                multiply(l, g * TG + k)

        drain(l)
        finish(l)
        if l == 0:
            g_finish(1)


def solution(mesh):
    pair_spec = P(('batch', 'dap'), None, None)
    mask_spec = P(('batch', 'dap'), None)
    msa_spec = P(None, ('batch', 'dap'), None)
    vm = pl.BlockSpec(memory_space=pltpu.VMEM)
    dma = pltpu.SemaphoreType.DMA

    def bf(*shape):
        return pltpu.VMEM(shape, BF16)

    def f3(*shape):
        return pltpu.VMEM(shape, F32)

    call = pl.pallas_call(
        kernel,
        out_shape=jax.ShapeDtypeStruct((16, W2, W), BF16),
        in_specs=[vm] * 16,
        out_specs=vm,
        scratch_shapes=[
            bf(2, 8, W, W2), bf(NL, 1024, W), bf(NL, 16, 16, W), bf(NL, 512, W), bf(NL, 64, W2),
            f3(NL, W, 16), f3(NL, 2, W, W), f3(2, 8, 1, W2),
            bf(NL, 16, W2, W), bf(8, 1024, W2),
            bf(NL, W, 1024), bf(NL, NT, 4 * CC, W), bf(NL, W, W), bf(NL, W, W),
            bf(2, 8, W, W2), bf(W2, W2),
            bf(NL, 2, NT, W2, W), bf(NL, 2, NT, W2, W), bf(NL, NZ, 2, 2, NT, W2, W),
            f3(NL, 2, NT, W2, W), f3(NL, NT, W2, W), bf(W2, W2), bf(2, 8, W, W2),
            dma((NL, 8)), dma((NL, 8)), dma((NL, 8)), dma((NL, 8)), dma((NL,)),
            dma((NL, NG, 2)), dma((NL, NG, 2)),
            dma((NL, 2, NZ - 1, NG, 2)), dma((NL, 2, NZ - 1, NG, 2)),
            dma((NL, NZ, NG, 2)), dma((NL, NZ, NG, 2)),
            dma((NL, NT)), dma((NL, NT)),
        ],
        compiler_params=pltpu.CompilerParams(collective_id=0, has_side_effects=True),
        name='layers',
    )

    def device_fn(pair, mask, msa, opm_norm, opm_w_in, opm_b_in, opm_w_out, opm_b_out, tri_norm_in, tri_w_ab, tri_b_ab,
                  tri_w_gate, tri_b_gate, tri_norm_out, tri_w_out, tri_b_out):
        return call(pair, mask, msa.transpose(1, 0, 2), opm_w_in.reshape(2, W2, 64), opm_norm, opm_b_in,
                    opm_w_out, tri_w_ab.reshape(2, W, 512), tri_w_gate, tri_w_out,
                    opm_b_out, tri_norm_in, tri_b_out, tri_b_gate, tri_b_ab, tri_norm_out)

    return jax.shard_map(device_fn, mesh=mesh, in_specs=(pair_spec, mask_spec, msa_spec) + (P(),) * 13,
                         out_specs=pair_spec, check_vma=False)
```
